512 devices in a mesh: gx: 32 (over z_hi, x, core), gy: 16 (over z_lo, y).
Axes of the slice: x: 4, y: 8, z: 8 (z_hi: 4, z_lo: 2; z = z_hi * 2 + z_lo), core: 2. Of those that a mesh axis runs over, the one named last changes fastest.
Arguments:
- core_one: bfloat16 [200, 128], replicated, may hold values from -6 to 6
- core_two: bfloat16 [200, 4096], replicated, may hold values from -1 to 1
- core_three: bfloat16 [250, 256], replicated, may hold values from -1 to 1
- dense_rows: bfloat16 [32768, 128], P(('gx', 'gy')), may hold values from -24 to 24
- w_top: bfloat16 [256, 256], replicated, may hold values from -0.375 to 0.375
- bias_top: float32 [256], replicated, may hold values from -3 to 3
- w_out: float32 [256], replicated, may hold values from -0.75 to 0.75
- labels: int32 [32768], P(('gx', 'gy')), may hold values 0 or 1
- bag_ids: int32 [512, 256], P(('gx', 'gy')), may hold values from 0 to 63, never falling along the last dimension, each value on 1 to 8 neighbouring positions
- digit_one: int32 [512, 256], P(('gx', 'gy')), may hold values from 0 to 199
- digit_two: int32 [512, 256], P(('gx', 'gy')), may hold values from 0 to 199
- digit_three: int32 [512, 256], P(('gx', 'gy')), may hold values from 0 to 249
Outputs:
- core_grad: float32 [908800], P(('gx', 'gy'))
- top_grad: float32 [258, 256], replicated
The draws below stay inside these ranges and needn't reach their ends.
Inputs may be any that keep to these rules, and one draw needn't show every extreme that they name: `bag_ids`: along a row, never falling; every sample of the block gets 1 to 8 lookups, one exactly 8.
All inputs are finite; a program needn't handle non-finite values. No bound on the sum of `labels` on one device may be relied on, other than what follows from the above.
Results may differ from the reference program's by a relative error of at most 0.0018.
The reference program's roundings to bfloat16 on the way (of `joined` and `dpre`) count: a program that leaves them out, or rounds other values in their place, can miss the bound.
Values sent between devices are 32-bit elements; how exact they have to be, the bound alone decides.
A program may use at most 64 MiB of HBM per device.

```python
import math
import jax
import jax.numpy as jnp
import numpy as np
from jax import lax

N1 = 200
N2 = 200
N3 = 250
D1 = 4
D2 = 4
D3 = 8
R = 32
HID = 256
BAG_MOST = 8
BATCH_DEV = 64
DIM = 128
LOOKS = 256
BATCH = 32768
N_GX = 32
N_GY = 16
DEVICES = 512


def touch_ends(drawn, rng, low, largest):
    longest = drawn.shape.index(max(drawn.shape))
    spots = []
    for shift in (0, 1):
        where = [jax.random.randint(jax.random.fold_in(rng, axis), (), 0, length) for axis, length in enumerate(drawn.shape)]
        where[longest] = (where[longest] + shift) % drawn.shape[longest]
        spots.append(tuple(where))
    return drawn.at[spots[0]].set(low).at[spots[1]].set(largest)


def spiked(array, stream_key, source, target, blocks, factor):
    owner, partner = [(jnp.arange(array.shape[position]) // (array.shape[position] // blocks)).reshape([-1 if axis == position else 1 for axis in range(array.ndim)]) for position in (source, target)]
    chosen = jax.random.permutation(stream_key, blocks)[partner]
    strong = (owner == chosen) | (owner == (partner + blocks // 2) % blocks)
    return jnp.where(strong, factor * array, array)


def levels(stream_key, dims, cuts, smallest, top_value):
    def one(dim, shards_of):
        steps = jax.random.uniform(jax.random.fold_in(jax.random.fold_in(stream_key, 6), dim), (shards_of,), jnp.float32, smallest / len(cuts), top_value / len(cuts))
        return jnp.repeat(jnp.exp(steps), dims[dim] // shards_of).reshape((-1,) + (1,) * (len(dims) - dim - 1))

    factor_of = one(*cuts[0])
    for cut in cuts[1:]:
        factor_of = factor_of * one(*cut)
    return factor_of


def split_up(amount, total, reach, slope):
    loads = [(1 << 20) // math.isqrt(standing ** slope) + 1 for standing in range(2, amount + 1)]
    spare, given = total - reach - (amount - 1), [1] * (amount - 1)
    while spare > 0:
        movable = [i for i in range(amount - 1) if given[i] < reach]
        pool, left = sum([loads[i] for i in movable]), spare
        for i in movable:
            more = min(reach - given[i], max(1, left * loads[i] // pool), spare)
            given[i] = given[i] + more
            spare = spare - more
    return np.array([reach] + given)


def uneven_parts(key, number_of, total, reach, slope):
    if number_of == 2:
        one = jax.random.randint(key, (), max(1, total - reach), min(reach, total - 1) + 1)
        return jnp.stack([one, total - one])
    sizes = jnp.asarray(split_up(number_of, total, reach, slope), jnp.int32)
    pairs = (number_of - 1) // 2
    giver, receiver = sizes[1:1 + 2 * pairs:2], sizes[2:2 + 2 * pairs:2]
    room = jnp.minimum(giver - 1, reach - receiver)
    passed = jax.random.randint(jax.random.fold_in(key, 1), (pairs,), 0, 1 << 20) % (room + 1)
    sizes = sizes.at[1:1 + 2 * pairs:2].set(giver - passed).at[2:2 + 2 * pairs:2].set(receiver + passed)
    return sizes[jax.random.permutation(jax.random.fold_in(key, 2), number_of)]


def bell_draw(stream_key, shape, spread, most, cuts=(), kind=jnp.bfloat16):
    level = levels(stream_key, shape, cuts, -0.22, 0.18) if cuts else 1.0
    array = jax.random.normal(stream_key, shape, jnp.float32) * spread * level
    return jnp.minimum(jnp.maximum(array, -most), most).astype(kind)


def heavy_noise(key, shape, width, limit, cuts, heavy, held_as=jnp.bfloat16):
    result = width * jax.random.normal(key, shape, jnp.float32)
    if cuts:
        result = result * levels(key, shape, cuts, -0.22, 0.18)
    return jnp.clip(spiked(result, jax.random.fold_in(key, 3), *heavy), -limit, limit).astype(held_as)


def setup_inputs(seed: int = 0) -> dict:
    keys = jax.random.split(jax.random.key(seed), 13)
    core_one = bell_draw(keys[0], (N1, D1 * R), 1.0, 6.0)
    core_two = bell_draw(keys[1], (N2, R * D2 * R), R ** -0.5, 1.0)
    core_three = bell_draw(keys[2], (N3, R * D3), R ** -0.5, 1.0)
    dense_rows = heavy_noise(keys[3], (BATCH, DIM), 1.0, 24.0, ((0, 512),), (0, 1, 128, 5.5))
    w_top = bell_draw(keys[4], (2 * DIM, HID), (2 * DIM) ** -0.5, 0.375)
    bias_top = bell_draw(keys[5], (HID,), 0.5, 3.0, (), jnp.float32)
    w_out = bell_draw(keys[6], (HID,), (HID // 4) ** -0.5, 0.75, (), jnp.float32)
    labels = touch_ends((jax.random.randint(keys[7], (BATCH,), 0, 4) < 1).astype(jnp.int32), jax.random.fold_in(keys[7], 1), 0, 1)
    bag_ids = jax.vmap(lambda own: jnp.searchsorted(jnp.cumsum(uneven_parts(own, BATCH_DEV, LOOKS, BAG_MOST, 1)), jnp.arange(LOOKS), side="right"))(jax.random.split(keys[8], DEVICES)).reshape((DEVICES, LOOKS)).astype(jnp.int32)
    digit_one = touch_ends(jax.random.randint(keys[9], (DEVICES, LOOKS), 0, N1), jax.random.fold_in(keys[9], 1), 0, N1 - 1).astype(jnp.int32)
    digit_two = touch_ends(jax.random.randint(keys[10], (DEVICES, LOOKS), 0, N2), jax.random.fold_in(keys[10], 1), 0, N2 - 1).astype(jnp.int32)
    digit_three = touch_ends(jax.random.randint(keys[11], (DEVICES, LOOKS), 0, N3), jax.random.fold_in(keys[11], 1), 0, N3 - 1).astype(jnp.int32)
    return {"core_one": core_one, "core_two": core_two, "core_three": core_three, "dense_rows": dense_rows, "w_top": w_top, "bias_top": bias_top, "w_out": w_out, "labels": labels, "bag_ids": bag_ids, "digit_one": digit_one, "digit_two": digit_two, "digit_three": digit_three}


def reference(core_one, core_two, core_three, dense_rows, w_top, bias_top, w_out, labels, bag_ids, digit_one, digit_two, digit_three):
    high = lax.Precision.HIGHEST
    groups = N_GX * N_GY
    dense_view = dense_rows.reshape(groups, BATCH_DEV, DIM)
    label_view = labels.reshape(groups, BATCH_DEV)

    def device_terms(carry, item):
        dense_block, label_block, bags, first_digit, second_digit, third_digit = item
        first = core_one[first_digit].astype(jnp.float32).reshape(-1, D1, R)
        middle = core_two[second_digit].astype(jnp.float32).reshape(-1, R, D2 * R)
        last = core_three[third_digit].astype(jnp.float32).reshape(-1, R, D3)
        left = jnp.einsum("nia,nab->nib", first, middle, precision=high).reshape(-1, D1 * D2, R)
        embedded = jnp.einsum("npa,nad->npd", left, last, precision=high).reshape(-1, D1 * D2 * D3)
        pooled = jax.ops.segment_sum(embedded, bags, num_segments=BATCH_DEV)
        joined = jnp.concatenate([dense_block, pooled.astype(jnp.bfloat16)], axis=1)
        pre = jnp.dot(joined, w_top, preferred_element_type=jnp.float32) + bias_top[None, :]
        sig = jax.nn.sigmoid(pre)
        hidden = pre * sig
        logit = jnp.dot(hidden, w_out, precision=high)
        dlogit = (jax.nn.sigmoid(logit) - label_block.astype(jnp.float32)) / BATCH_DEV
        dpre = dlogit[:, None] * w_out[None, :] * (sig * (1.0 + pre * (1.0 - sig)))
        dpre_low = dpre.astype(jnp.bfloat16)
        grad_weight = jnp.dot(joined.T, dpre_low, preferred_element_type=jnp.float32)
        grad_bias = jnp.sum(dpre, axis=0)
        grad_output = jnp.sum(hidden * dlogit[:, None], axis=0)
        top_local = jnp.concatenate([grad_weight, grad_bias[None, :], grad_output[None, :]], axis=0)
        grad_pooled = jnp.dot(dpre_low, w_top[D1 * D2 * D3:].T, preferred_element_type=jnp.float32)
        grad_view = grad_pooled[bags].reshape(-1, D1 * D2, D3)
        grad_last = jnp.einsum("npa,npd->nad", left, grad_view, precision=high)
        grad_left = jnp.einsum("npd,nad->npa", grad_view, last, precision=high).reshape(-1, D1, D2 * R)
        grad_first = jnp.einsum("nib,nab->nia", grad_left, middle, precision=high)
        grad_middle = jnp.einsum("nia,nib->nab", first, grad_left, precision=high)
        sum_first = jax.ops.segment_sum(grad_first.reshape(-1, D1 * R), first_digit, num_segments=N1)
        sum_middle = jax.ops.segment_sum(grad_middle.reshape(-1, R * D2 * R), second_digit, num_segments=N2)
        sum_last = jax.ops.segment_sum(grad_last.reshape(-1, R * D3), third_digit, num_segments=N3)
        return (carry[0] + sum_first, carry[1] + sum_middle, carry[2] + sum_last, carry[3] + top_local), None

    start = (jnp.zeros((N1, D1 * R), jnp.float32), jnp.zeros((N2, R * D2 * R), jnp.float32),
             jnp.zeros((N3, R * D3), jnp.float32), jnp.zeros((2 * D1 * D2 * D3 + 2, HID), jnp.float32))
    totals, _ = lax.scan(device_terms, start, (dense_view, label_view, bag_ids, digit_one, digit_two, digit_three))
    core_grad = jnp.concatenate([totals[0].reshape(-1), totals[1].reshape(-1), totals[2].reshape(-1)])
    return core_grad, totals[3]
```

```python
import functools

import jax
import jax.numpy as jnp
from jax import lax
from jax.experimental import pallas as pl
from jax.experimental.pallas import tpu as pltpu
from jax.sharding import PartitionSpec as P

D1 = 4
D2 = 4
D3 = 8
R = 32


def one_hot(digits, count, kind):
    return (digits[:, None] == jnp.arange(count, dtype=jnp.int32)[None, :]).astype(kind)


def slices(digits, core):
    return jnp.dot(
        one_hot(digits, core.shape[0], jnp.bfloat16), core, preferred_element_type=jnp.float32
    )


def factors(digits, cores):
    high = lax.Precision.HIGHEST
    first = slices(digits[0], cores[0]).reshape(-1, D1, R)
    middle = slices(digits[1], cores[1]).reshape(-1, R, D2 * R)
    last = slices(digits[2], cores[2]).reshape(-1, R, D3)
    left = jnp.einsum("nia,nab->nib", first, middle, precision=high).reshape(-1, D1 * D2, R)
    return (first, middle, last, left)


MESH = pl.DeviceIdType.MESH
ORDER = (1, 7, 2, 6, 3, 5, 4)
XORDER = (1, 3, 2)


def whereabouts():
    gx, gy = lax.axis_index("gx"), lax.axis_index("gy")
    core, x = gx % 2, (gx // 2) % 4
    y, z = gy % 8, (gx // 8) * 2 + gy // 8
    u = (1 - core) * y + core * z
    v = (1 - core) * z + core * y
    return core, x, u, v


def place(core, x, u, v):
    y = (1 - core) * u + core * v
    z = core * u + (1 - core) * v
    return ((z // 2) * 8 + x * 2 + core, (z % 2) * 8 + y)


def summed(rows, step, store, *parts):
    def body(i, carry):
        at = pl.ds(pl.multiple_of(i * step, step), step)
        total = parts[0](at)
        for part in parts[1:]:
            total = total + part(at)
        store(at, total)
        return carry

    lax.fori_loop(0, rows // step, body, 0)


def exchange_kernel(w, t, e, out, top, r0, s1, r1a, r1b, s2a, s2b, r2a, r2b, s3a, s3b, r3a, r3b,
                    rt0, re0, st1, rt1, st2, rt2, rt3, g1, g2, g3, send, recv):
    core, x, u, v = whereabouts()
    y = (1 - core) * u + core * v
    z = core * u + (1 - core) * v
    mate = ((z // 2) * 8 + x * 2 + (1 - core), (z % 2) * 8 + y)
    other_x = {k: place(core, (x + k) % 4, u, v) for k in XORDER}
    other_u = {k: place(core, x, (u + k) % 8, v) for k in ORDER}
    other_v = {k: place(core, x, u, (v + k) % 8) for k in ORDER}
    barrier = pltpu.get_barrier_semaphore()
    peers = [mate] + list(other_x.values()) + list(other_u.values()) + list(other_v.values())
    for peer in peers:
        pl.semaphore_signal(barrier, inc=1, device_id=peer, device_id_type=MESH)
    pl.semaphore_wait(barrier, len(peers))
    copies = []

    def put(src, dst, peer):
        spot = len(copies)
        copy = pltpu.make_async_remote_copy(
            src_ref=src, dst_ref=dst, send_sem=send.at[spot], recv_sem=recv.at[spot],
            device_id=peer, device_id_type=MESH)
        copy.start()
        copies.append(copy)
        return copy

    def arrived(group):
        for copy in group:
            copy.wait_recv()

    t0 = [put(t.at[1 - core], rt0, mate), put(e, re0, mate)]
    p0 = [put(w.at[1 - core, color], r0.at[color], mate) for color in (0, 1)]
    arrived(t0)
    extra = e[...] + re0[...]
    for part in range(4):
        rows = pl.ds(part * 64, 64)
        st1[part, 0:64, :] = t[core, rows, :] + rt0[rows, :]
        st1[part, 64:72, :] = extra
    t1 = [put(st1.at[(x + k) % 4], rt1.at[x], other_x[k]) for k in XORDER]
    rt1[x] = st1[x]

    def fold(color):
        def store(at, value):
            s1[color, at, :] = value
        summed(2048, 256, store, lambda at: w[core, color, at, :], lambda at: r0[color, at, :])

    arrived(p0[:1])
    fold(0)
    p1a = [put(s1.at[0, pl.ds(((x + k) % 4) * 512, 512)], r1a.at[k - 1], other_x[k]) for k in XORDER]
    arrived(p0[1:])
    fold(1)
    p1b = [put(s1.at[1, pl.ds(((u + k) % 8) * 256, 256)], r1b.at[k - 1], other_u[k]) for k in ORDER]

    arrived(t1)
    total = rt1[0]
    for part in range(1, 4):
        total = total + rt1[part]
    for part in range(8):
        st2[part, 0:8, :] = total[part * 8:part * 8 + 8]
        st2[part, 8:16, :] = total[64:72]
    t2 = [put(st2.at[(v + k) % 8], rt2.at[v], other_v[k]) for k in ORDER]
    rt2[v] = st2[v]
    arrived(t2)
    total = rt2[0]
    for part in range(1, 8):
        total = total + rt2[part]
    rt3[u] = total
    t3 = [put(rt3.at[u], rt3.at[u], other_u[k]) for k in ORDER]

    arrived(p1a)

    def store2a(at, value):
        s2a[at, :] = value

    summed(512, 128, store2a, lambda at: s1[0, pl.ds(x * 512 + at.start, at.size), :],
           *[functools.partial(lambda k, at: r1a[k, at, :], k) for k in range(3)])
    p2a = [put(s2a.at[pl.ds(((u + k) % 8) * 64, 64)], r2a.at[k - 1], other_u[k]) for k in ORDER]
    arrived(p1b)

    def store2b(at, value):
        s2b[at, :] = value

    summed(256, 64, store2b, lambda at: s1[1, pl.ds(u * 256 + at.start, at.size), :],
           *[functools.partial(lambda k, at: r1b[k, at, :], k) for k in range(7)])
    p2b = [put(s2b.at[pl.ds(((v + k) % 8) * 32, 32)], r2b.at[k - 1], other_v[k]) for k in ORDER]

    arrived(t3)
    total = rt3[0]
    for part in range(1, 8):
        total = total + rt3[part]
    g1[v] = total[0:8]
    extra = total[8:16]
    t4 = [put(g1.at[v], g1.at[v], other_v[k]) for k in ORDER]

    arrived(p2a)
    total = s2a[pl.ds(u * 64, 64), :]
    for part in range(7):
        total = total + r2a[part]
    s3a[...] = total
    p3a = [put(s3a.at[pl.ds(((v + k) % 8) * 8, 8)], r3a.at[k - 1], other_v[k]) for k in ORDER]
    arrived(p2b)
    total = s2b[pl.ds(v * 32, 32), :]
    for part in range(7):
        total = total + r2b[part]
    s3b[...] = total
    p3b = [put(s3b.at[pl.ds(((x + k) % 4) * 8, 8)], r3b.at[k - 1], other_x[k]) for k in XORDER]

    arrived(t4)
    g2[x] = g1[...]
    t5 = [put(g2.at[x], g2.at[x], other_x[k]) for k in XORDER]
    for copy in t5:
        copy.wait_recv()
    t6 = put(g2, g3, mate)

    arrived(p3a)
    upper = s3a[pl.ds(v * 8, 8), :]
    for part in range(7):
        upper = upper + r3a[part]
    arrived(p3b)
    lower = s3b[pl.ds(x * 8, 8), :]
    for part in range(3):
        lower = lower + r3b[part]
    gx, gy = lax.axis_index("gx"), lax.axis_index("gy")
    offset = ((gx * 16 + gy) * 1775) % 128
    turned = pltpu.roll(jnp.concatenate([upper, lower], axis=0), (128 - offset) % 128, 1)
    below = pltpu.roll(turned, 15, 0)
    lane = lax.broadcasted_iota(jnp.int32, (16, 128), 1)
    out[...] = jnp.where(lane < 128 - offset, turned, below)

    top[256:257, 0:128] = extra[0:1]
    top[256:257, 128:256] = extra[1:2]
    top[257:258, 0:128] = extra[2:3]
    top[257:258, 128:256] = extra[3:4]
    arrived([t6])

    @pl.when(core == 0)
    def _():
        top[0:256, 0:128] = g2[...].reshape(256, 128)
        top[0:256, 128:256] = g3[...].reshape(256, 128)

    @pl.when(core == 1)
    def _():
        top[0:256, 128:256] = g2[...].reshape(256, 128)
        top[0:256, 0:128] = g3[...].reshape(256, 128)

    for copy in copies:
        copy.wait_send()


def exchange(w, t, e):
    f32 = jnp.float32
    shapes = [(2, 2048), (2, 2048), (3, 512), (7, 256), (512,), (256,), (7, 64), (7, 32), (64,), (32,), (7, 8), (3, 8),
              (256,), (8,), (4, 72), (4, 72), (8, 16), (8, 16), (8, 16), (8, 8), (4, 8, 8), (4, 8, 8)]
    vmem = pl.BlockSpec(memory_space=pltpu.VMEM)
    return pl.pallas_call(
        exchange_kernel,
        out_shape=(jax.ShapeDtypeStruct((16, 128), f32), jax.ShapeDtypeStruct((258, 256), f32)),
        in_specs=[vmem] * 3,
        out_specs=(vmem, vmem),
        scratch_shapes=[pltpu.VMEM(shape + (128,), f32) for shape in shapes]
        + [pltpu.SemaphoreType.DMA((70,)), pltpu.SemaphoreType.DMA((70,))],
        compiler_params=pltpu.CompilerParams(collective_id=0, has_side_effects=True, vmem_limit_bytes=40 * 1024 * 1024),
        name="exchange",
    )(w, t, e)


def pack_kernel(flat, w):
    def body(q, carry):
        b, x, y = (q // 16) % 2, (q // 32) % 4, q % 8
        z = (q // 128) * 2 + (q // 8) % 2
        u = (1 - b) * y + b * z
        v = (1 - b) * z + b * y
        rows = flat[pl.ds((1775 * q) // 128, 16), :]
        w[b, 0, pl.ds(pl.multiple_of((x * 64 + u * 8 + v) * 8, 8), 8), :] = rows[0:8]
        w[b, 1, pl.ds(pl.multiple_of((u * 32 + v * 4 + x) * 8, 8), 8), :] = rows[8:16]
        return carry

    lax.fori_loop(0, 512, body, 0)


def pack(flat):
    vmem = pl.BlockSpec(memory_space=pltpu.VMEM)
    return pl.pallas_call(
        pack_kernel,
        out_shape=jax.ShapeDtypeStruct((2, 2, 2048, 128), jnp.float32),
        in_specs=[vmem],
        out_specs=vmem,
        compiler_params=pltpu.CompilerParams(vmem_limit_bytes=20 * 1024 * 1024),
        name="pack",
    )(flat)


def per_device(
    core_one,
    core_two,
    core_three,
    dense_rows,
    w_top,
    bias_top,
    w_out,
    labels,
    bag_ids,
    digit_one,
    digit_two,
    digit_three,
):
    high = lax.Precision.HIGHEST
    cores = (core_one, core_two, core_three)
    digits = jnp.stack([digit_one[0], digit_two[0], digit_three[0]])
    looks = digits.shape[1]
    block = min(256, looks)
    blocks = looks // block
    blocked = digits.reshape(3, blocks, block).transpose(1, 0, 2)
    width = D1 * D2 * D3

    def forward(carry, part):
        first, middle, last, left = factors(part, cores)
        return (carry, jnp.einsum("npa,nad->npd", left, last, precision=high).reshape(block, width))

    _, embedded = lax.scan(forward, jnp.zeros((), jnp.float32), blocked)
    embedded = embedded.reshape(looks, width)
    samples = dense_rows.shape[0]
    bag_table = one_hot(bag_ids[0], samples, jnp.float32)
    pooled = jnp.dot(bag_table.T, embedded, precision=high)
    joined = jnp.concatenate([dense_rows, pooled.astype(jnp.bfloat16)], axis=1)
    pre = jnp.dot(joined, w_top, preferred_element_type=jnp.float32) + bias_top[None, :]
    sig = jax.nn.sigmoid(pre)
    hidden = pre * sig
    logit = jnp.dot(hidden, w_out, precision=high)
    dlogit = (jax.nn.sigmoid(logit) - labels.astype(jnp.float32)) / samples
    dpre = dlogit[:, None] * w_out[None, :] * (sig * (1.0 + pre * (1.0 - sig)))
    dpre_low = dpre.astype(jnp.bfloat16)
    grad_weight = jnp.dot(joined.T, dpre_low, preferred_element_type=jnp.float32)
    grad_bias = jnp.sum(dpre, axis=0)
    grad_output = jnp.sum(hidden * dlogit[:, None], axis=0)
    top_local = jnp.concatenate([grad_weight, grad_bias[None, :], grad_output[None, :]], axis=0)
    grad_pooled = jnp.dot(dpre_low, w_top[width:].T, preferred_element_type=jnp.float32)
    grad_embedded = jnp.dot(bag_table, grad_pooled, precision=high).reshape(blocks, block, width)

    def backward(totals, inputs):
        part, grad_block = inputs
        first, middle, last, left = factors(part, cores)
        grad_view = grad_block.reshape(block, D1 * D2, D3)
        grad_last = jnp.einsum("npa,npd->nad", left, grad_view, precision=high)
        grad_left = jnp.einsum("npd,nad->npa", grad_view, last, precision=high).reshape(
            block, D1, D2 * R
        )
        grad_first = jnp.einsum("nib,nab->nia", grad_left, middle, precision=high)
        grad_middle = jnp.einsum("nia,nib->nab", first, grad_left, precision=high)
        pieces = (
            grad_first.reshape(block, -1),
            grad_middle.reshape(block, -1),
            grad_last.reshape(block, -1),
        )
        updated = tuple(
            (
                total
                + jnp.dot(
                    one_hot(part[number], cores[number].shape[0], jnp.float32).T,
                    pieces[number],
                    precision=high,
                )
                for number, total in enumerate(totals)
            )
        )
        return (updated, None)

    start = tuple((jnp.zeros(core.shape, jnp.float32) for core in cores))
    totals, _ = lax.scan(backward, start, (blocked, grad_embedded))
    flat = jnp.concatenate([total.reshape(-1) for total in totals])
    packed = pack(jnp.pad(flat, (0, 512)).reshape(7104, 128))
    sides = jnp.stack([top_local[:256, :128], top_local[:256, 128:]])
    extra = jnp.pad(top_local[256:].reshape(4, 128), ((0, 4), (0, 0)))
    chunk, top_grad = exchange(packed, sides, extra)
    return (chunk.reshape(-1)[:1775], top_grad)


def solution(mesh):
    return jax.shard_map(
        per_device,
        mesh=mesh,
        in_specs=(
            P(),
            P(),
            P(),
            P(("gx", "gy"), None),
            P(),
            P(),
            P(),
            P(("gx", "gy")),
            P(("gx", "gy"), None),
            P(("gx", "gy"), None),
            P(("gx", "gy"), None),
            P(("gx", "gy"), None),
        ),
        out_specs=(P(("gx", "gy")), P()),
        check_vma=False,
    )
```

```python
import functools

import jax
import jax.numpy as jnp
from jax import lax
from jax.experimental import pallas as pl
from jax.experimental.pallas import tpu as pltpu
from jax.sharding import PartitionSpec as P

MESH = pl.DeviceIdType.MESH
ORDER = (1, 7, 2, 6, 3, 5, 4)
XORDER = (1, 3, 2)


def whereabouts():
    gx, gy = lax.axis_index("gx"), lax.axis_index("gy")
    core, x = gx % 2, (gx // 2) % 4
    y, z = gy % 8, (gx // 8) * 2 + gy // 8
    u = (1 - core) * y + core * z
    v = (1 - core) * z + core * y
    return core, x, u, v


def place(core, x, u, v):
    y = (1 - core) * u + core * v
    z = core * u + (1 - core) * v
    return ((z // 2) * 8 + x * 2 + core, (z % 2) * 8 + y)


def summed(rows, step, store, *parts):
    def body(i, carry):
        at = pl.ds(pl.multiple_of(i * step, step), step)
        total = parts[0](at)
        for part in parts[1:]:
            total = total + part(at)
        store(at, total)
        return carry

    lax.fori_loop(0, rows // step, body, 0)


def exchange_kernel(w, t, e, out, top, r0, s1, r1a, r1b, s2a, s2b, r2a, r2b, s3a, s3b, r3a, r3b,
                    rt0, re0, st1, rt1, st2, rt2, rt3, g1, g2, g3, send, recv):
    core, x, u, v = whereabouts()
    y = (1 - core) * u + core * v
    z = core * u + (1 - core) * v
    mate = ((z // 2) * 8 + x * 2 + (1 - core), (z % 2) * 8 + y)
    other_x = {k: place(core, (x + k) % 4, u, v) for k in XORDER}
    other_u = {k: place(core, x, (u + k) % 8, v) for k in ORDER}
    other_v = {k: place(core, x, u, (v + k) % 8) for k in ORDER}
    barrier = pltpu.get_barrier_semaphore()
    peers = [mate] + list(other_x.values()) + list(other_u.values()) + list(other_v.values())
    for peer in peers:
        pl.semaphore_signal(barrier, inc=1, device_id=peer, device_id_type=MESH)
    pl.semaphore_wait(barrier, len(peers))
    copies = []

    def put(src, dst, peer):
        spot = len(copies)
        copy = pltpu.make_async_remote_copy(
            src_ref=src, dst_ref=dst, send_sem=send.at[spot], recv_sem=recv.at[spot],
            device_id=peer, device_id_type=MESH)
        copy.start()
        copies.append(copy)
        return copy

    def arrived(group):
        for copy in group:
            copy.wait_recv()

    t0 = [put(t.at[1 - core], rt0, mate), put(e, re0, mate)]
    p0 = [put(w.at[1 - core, color], r0.at[color], mate) for color in (0, 1)]
    arrived(t0)
    extra = e[...] + re0[...]
    for part in range(4):
        rows = pl.ds(part * 64, 64)
        st1[part, 0:64, :] = t[core, rows, :] + rt0[rows, :]
        st1[part, 64:72, :] = extra
    t1 = [put(st1.at[(x + k) % 4], rt1.at[x], other_x[k]) for k in XORDER]
    rt1[x] = st1[x]

    def fold(color):
        def store(at, value):
            s1[color, at, :] = value
        summed(2048, 256, store, lambda at: w[core, color, at, :], lambda at: r0[color, at, :])

    arrived(p0[:1])
    fold(0)
    p1a = [put(s1.at[0, pl.ds(((x + k) % 4) * 512, 512)], r1a.at[k - 1], other_x[k]) for k in XORDER]
    arrived(p0[1:])
    fold(1)
    p1b = [put(s1.at[1, pl.ds(((u + k) % 8) * 256, 256)], r1b.at[k - 1], other_u[k]) for k in ORDER]

    arrived(t1)
    total = rt1[0]
    for part in range(1, 4):
        total = total + rt1[part]
    for part in range(8):
        st2[part, 0:8, :] = total[part * 8:part * 8 + 8]
        st2[part, 8:16, :] = total[64:72]
    t2 = [put(st2.at[(v + k) % 8], rt2.at[v], other_v[k]) for k in ORDER]
    rt2[v] = st2[v]
    arrived(t2)
    total = rt2[0]
    for part in range(1, 8):
        total = total + rt2[part]
    rt3[u] = total
    t3 = [put(rt3.at[u], rt3.at[u], other_u[k]) for k in ORDER]

    arrived(p1a)

    def store2a(at, value):
        s2a[at, :] = value

    summed(512, 128, store2a, lambda at: s1[0, pl.ds(x * 512 + at.start, at.size), :],
           *[functools.partial(lambda k, at: r1a[k, at, :], k) for k in range(3)])
    p2a = [put(s2a.at[pl.ds(((u + k) % 8) * 64, 64)], r2a.at[k - 1], other_u[k]) for k in ORDER]
    arrived(p1b)

    def store2b(at, value):
        s2b[at, :] = value

    summed(256, 64, store2b, lambda at: s1[1, pl.ds(u * 256 + at.start, at.size), :],
           *[functools.partial(lambda k, at: r1b[k, at, :], k) for k in range(7)])
    p2b = [put(s2b.at[pl.ds(((v + k) % 8) * 32, 32)], r2b.at[k - 1], other_v[k]) for k in ORDER]

    arrived(t3)
    total = rt3[0]
    for part in range(1, 8):
        total = total + rt3[part]
    g1[v] = total[0:8]
    extra = total[8:16]
    t4 = [put(g1.at[v], g1.at[v], other_v[k]) for k in ORDER]

    arrived(p2a)
    total = s2a[pl.ds(u * 64, 64), :]
    for part in range(7):
        total = total + r2a[part]
    s3a[...] = total
    p3a = [put(s3a.at[pl.ds(((v + k) % 8) * 8, 8)], r3a.at[k - 1], other_v[k]) for k in ORDER]
    arrived(p2b)
    total = s2b[pl.ds(v * 32, 32), :]
    for part in range(7):
        total = total + r2b[part]
    s3b[...] = total
    p3b = [put(s3b.at[pl.ds(((x + k) % 4) * 8, 8)], r3b.at[k - 1], other_x[k]) for k in XORDER]

    arrived(t4)
    g2[x] = g1[...]
    t5 = [put(g2.at[x], g2.at[x], other_x[k]) for k in XORDER]
    for copy in t5:
        copy.wait_recv()
    t6 = put(g2, g3, mate)

    arrived(p3a)
    upper = s3a[pl.ds(v * 8, 8), :]
    for part in range(7):
        upper = upper + r3a[part]
    arrived(p3b)
    lower = s3b[pl.ds(x * 8, 8), :]
    for part in range(3):
        lower = lower + r3b[part]
    gx, gy = lax.axis_index("gx"), lax.axis_index("gy")
    offset = ((gx * 16 + gy) * 1775) % 128
    turned = pltpu.roll(jnp.concatenate([upper, lower], axis=0), (128 - offset) % 128, 1)
    below = pltpu.roll(turned, 15, 0)
    lane = lax.broadcasted_iota(jnp.int32, (16, 128), 1)
    out[...] = jnp.where(lane < 128 - offset, turned, below)

    top[256:257, 0:128] = extra[0:1]
    top[256:257, 128:256] = extra[1:2]
    top[257:258, 0:128] = extra[2:3]
    top[257:258, 128:256] = extra[3:4]
    arrived([t6])

    @pl.when(core == 0)
    def _():
        top[0:256, 0:128] = g2[...].reshape(256, 128)
        top[0:256, 128:256] = g3[...].reshape(256, 128)

    @pl.when(core == 1)
    def _():
        top[0:256, 128:256] = g2[...].reshape(256, 128)
        top[0:256, 0:128] = g3[...].reshape(256, 128)

    for copy in copies:
        copy.wait_send()


def exchange(w, t, e):
    f32 = jnp.float32
    shapes = [(2, 2048), (2, 2048), (3, 512), (7, 256), (512,), (256,), (7, 64), (7, 32), (64,), (32,), (7, 8), (3, 8),
              (256,), (8,), (4, 72), (4, 72), (8, 16), (8, 16), (8, 16), (8, 8), (4, 8, 8), (4, 8, 8)]
    vmem = pl.BlockSpec(memory_space=pltpu.VMEM)
    return pl.pallas_call(
        exchange_kernel,
        out_shape=(jax.ShapeDtypeStruct((16, 128), f32), jax.ShapeDtypeStruct((258, 256), f32)),
        in_specs=[vmem] * 3,
        out_specs=(vmem, vmem),
        scratch_shapes=[pltpu.VMEM(shape + (128,), f32) for shape in shapes]
        + [pltpu.SemaphoreType.DMA((70,)), pltpu.SemaphoreType.DMA((70,))],
        compiler_params=pltpu.CompilerParams(collective_id=0, has_side_effects=True, vmem_limit_bytes=40 * 1024 * 1024),
        name="exchange",
    )(w, t, e)


def contract(a, b, left, right, **kw):
    return lax.dot_general(a, b, (((left,), (right,)), ((), ())), preferred_element_type=jnp.float32, **kw)


def halves(value):
    high = value.astype(jnp.bfloat16)
    return high, (value - high.astype(jnp.float32)).astype(jnp.bfloat16)


def grads_kernel(one, two, three, dense, w_top, bias, w_out, labels, bags, digit_one, digit_two, digit_three,
                 w, t, e, first, mid, last, turned, left, g, gl, gm, glast, flat, sided, gf):
    bf16, f32 = jnp.bfloat16, jnp.float32
    high = lax.Precision.HIGHEST

    def hot(row, count, kind):
        return (lax.broadcasted_iota(jnp.int32, (count, row.shape[1]), 0) == row).astype(kind)

    hot_one = hot(digit_one[...], 200, bf16)
    hot_two = hot(digit_two[...], 200, bf16)
    hot_three = hot(digit_three[...], 250, bf16)
    bag = hot(bags[...], 64, f32)
    first[...] = contract(one[...], hot_one, 0, 0)
    ends = contract(three[...], hot_three, 0, 0)
    last[...] = ends
    for side in range(2):
        sided[side] = ends[:, side * 128:side * 128 + 128]
        for d in range(8):
            turned[d * 32:d * 32 + 32, side * 128:side * 128 + 128] = sided.at[side][pl.ds(d, 32, stride=8), :]
    for part in range(8):
        mid[part * 512:part * 512 + 512, :] = contract(two[:, part * 512:part * 512 + 512], hot_two, 0, 0)

    for b in range(4):
        sums = [jnp.zeros((32, 256), f32) for _ in range(4)]
        for a in range(32):
            piece = mid[a * 128 + b * 32:a * 128 + b * 32 + 32, :]
            sums = [total + first[i * 32 + a:i * 32 + a + 1, :] * piece for i, total in enumerate(sums)]
        for i in range(4):
            left[(i * 4 + b) * 32:(i * 4 + b) * 32 + 32, :] = sums[i]
    rows = []
    for p in range(16):
        total = jnp.zeros((8, 256), f32)
        for a in range(32):
            total = total + left[p * 32 + a:p * 32 + a + 1, :] * last[a * 8:a * 8 + 8, :]
        rows.append(total)
    embedded = jnp.concatenate(rows, axis=0)

    pooled = contract(bag, embedded, 1, 1, precision=high)
    joined = jnp.concatenate([dense[...], pooled.astype(bf16)], axis=1)
    pre = jnp.dot(joined, w_top[...], preferred_element_type=f32) + bias[...]
    sig = jax.nn.sigmoid(pre)
    hidden = pre * sig
    logit = jnp.sum(hidden * w_out[...], axis=1, keepdims=True)
    square = lax.broadcasted_iota(jnp.int32, (64, 64), 0) == lax.broadcasted_iota(jnp.int32, (64, 64), 1)
    label = jnp.sum(jnp.where(square, labels[...].astype(f32), 0.0), axis=1, keepdims=True)
    dlogit = (jax.nn.sigmoid(logit) - label) / 64
    dpre = dlogit * w_out[...] * (sig * (1.0 + pre * (1.0 - sig)))
    low = dpre.astype(bf16)
    weight = contract(joined, low, 0, 0)
    t[0] = weight[:, 0:128]
    t[1] = weight[:, 128:256]
    grad_bias = jnp.sum(dpre, axis=0, keepdims=True)
    grad_out = jnp.sum(hidden * dlogit, axis=0, keepdims=True)
    e[...] = jnp.concatenate([grad_bias[:, :128], grad_bias[:, 128:], grad_out[:, :128], grad_out[:, 128:],
                              jnp.zeros((4, 128), f32)], axis=0)
    pooled_grad = contract(w_top[128:256, :], low, 1, 1)
    g[...] = jnp.dot(pooled_grad, bag, precision=high, preferred_element_type=f32)

    for a in range(32):
        total = jnp.zeros((8, 256), f32)
        for p in range(16):
            total = total + left[p * 32 + a:p * 32 + a + 1, :] * g[p * 8:p * 8 + 8, :]
        glast[a * 8:a * 8 + 8, :] = total
    for p in range(16):
        total = jnp.zeros((32, 256), f32)
        for d in range(8):
            total = total + g[p * 8 + d:p * 8 + d + 1, :] * turned[d * 32:d * 32 + 32, :]
        gl[p * 32:p * 32 + 32, :] = total

    def scatter(table, value):
        upper, lower = halves(value)
        return contract(table, upper, 1, 1) + contract(table, lower, 1, 1)

    for a in range(0, 32, 2):
        for half in range(2):
            c = a + half
            partial = [jnp.zeros((8, 256), f32) for _ in range(4)]
            for b in range(16):
                piece = mid[c * 128 + b * 8:c * 128 + b * 8 + 8, :]
                total = jnp.zeros((8, 256), f32)
                for i in range(4):
                    slope = gl[i * 128 + b * 8:i * 128 + b * 8 + 8, :]
                    total = total + first[i * 32 + c:i * 32 + c + 1, :] * slope
                    partial[i] = partial[i] + slope * piece
                gm[half * 128 + b * 8:half * 128 + b * 8 + 8, :] = total
            for i in range(4):
                for side in range(2):
                    gf.at[side][pl.ds(i * 32 + c, 8, stride=128), :] = partial[i][:, side * 128:side * 128 + 128]
        middle = scatter(hot_two, gm[...])
        flat[pl.ds(200 + a, 200, stride=32), :] = middle[:, 0:128]
        flat[pl.ds(201 + a, 200, stride=32), :] = middle[:, 128:256]
    spread = scatter(hot_one, jnp.concatenate([gf[0], gf[1]], axis=1))
    total = spread[:, 0:128]
    for part in range(1, 8):
        total = total + spread[:, part * 128:part * 128 + 128]
    flat[7096:7104, :] = jnp.zeros((8, 128), f32)
    flat[0:200, :] = total
    ending = scatter(hot_three, glast[...])
    flat[pl.ds(6600, 250, stride=2), :] = ending[:, 0:128]
    flat[pl.ds(6601, 250, stride=2), :] = ending[:, 128:256]

    for q in range(512):
        b, x, y = (q // 16) % 2, (q // 32) % 4, q % 8
        z = (q // 128) * 2 + (q // 8) % 2
        u, v = (y, z) if b == 0 else (z, y)
        start = (1775 * q) // 128
        w[b, 0, (x * 64 + u * 8 + v) * 8:(x * 64 + u * 8 + v) * 8 + 8, :] = flat[start:start + 8, :]
        w[b, 1, (u * 32 + v * 4 + x) * 8:(u * 32 + v * 4 + x) * 8 + 8, :] = flat[start + 8:start + 16, :]


def grads(*args):
    f32 = jnp.float32
    vmem = pl.BlockSpec(memory_space=pltpu.VMEM)
    rows = [128, 4096, 256, 256, 512, 128, 512, 256, 256]
    return pl.pallas_call(
        grads_kernel,
        out_shape=(jax.ShapeDtypeStruct((2, 2, 2048, 128), f32), jax.ShapeDtypeStruct((2, 256, 128), f32),
                   jax.ShapeDtypeStruct((8, 128), f32)),
        in_specs=[vmem] * len(args),
        out_specs=(vmem,) * 3,
        scratch_shapes=[pltpu.VMEM((count, 256), f32) for count in rows] + [pltpu.VMEM((7104, 128), f32), pltpu.VMEM((2, 256, 128), f32), pltpu.VMEM((2, 1024, 128), f32)],
        compiler_params=pltpu.CompilerParams(vmem_limit_bytes=50 * 1024 * 1024),
        name="grads",
    )(*args)


def per_device(core_one, core_two, core_three, dense_rows, w_top, bias_top, w_out, labels, bag_ids, digit_one, digit_two,
               digit_three):
    packed, sides, extra = grads(core_one, core_two, core_three, dense_rows, w_top, bias_top[None], w_out[None], labels[None],
                                 bag_ids, digit_one, digit_two, digit_three)
    chunk, top_grad = exchange(packed, sides, extra)
    return (chunk.reshape(-1)[:1775], top_grad)


def solution(mesh):
    return jax.shard_map(
        per_device,
        mesh=mesh,
        in_specs=(
            P(),
            P(),
            P(),
            P(("gx", "gy"), None),
            P(),
            P(),
            P(),
            P(("gx", "gy")),
            P(("gx", "gy"), None),
            P(("gx", "gy"), None),
            P(("gx", "gy"), None),
            P(("gx", "gy"), None),
        ),
        out_specs=(P(("gx", "gy")), P()),
        check_vma=False,
    )
```

```python
import functools

import jax
import jax.numpy as jnp
from jax import lax
from jax.experimental import pallas as pl
from jax.experimental.pallas import tpu as pltpu
from jax.sharding import PartitionSpec as P

MESH = pl.DeviceIdType.MESH
ORDER = (1, 7, 2, 6, 3, 5, 4)
XORDER = (1, 3, 2)


def whereabouts():
    gx, gy = lax.axis_index("gx"), lax.axis_index("gy")
    core, x = gx % 2, (gx // 2) % 4
    y, z = gy % 8, (gx // 8) * 2 + gy // 8
    u = (1 - core) * y + core * z
    v = (1 - core) * z + core * y
    return core, x, u, v


def place(core, x, u, v):
    y = (1 - core) * u + core * v
    z = core * u + (1 - core) * v
    return ((z // 2) * 8 + x * 2 + core, (z % 2) * 8 + y)


def summed(rows, step, store, *parts):
    def body(i, carry):
        at = pl.ds(pl.multiple_of(i * step, step), step)
        total = parts[0](at)
        for part in parts[1:]:
            total = total + part(at)
        store(at, total)
        return carry

    lax.fori_loop(0, rows // step, body, 0)


def contract(a, b, left, right, **kw):
    return lax.dot_general(a, b, (((left,), (right,)), ((), ())), preferred_element_type=jnp.float32, **kw)


def halves(value):
    high = value.astype(jnp.bfloat16)
    return high, (value - high.astype(jnp.float32)).astype(jnp.bfloat16)


def step_kernel(*refs):
    sources, (out, top), rest = refs[:12], refs[12:14], refs[14:]
    inputs, sems, rest = rest[:12], rest[12], rest[13:]
    one, two, three, dense, w_top, bias, w_out, labels, bags, digit_one, digit_two, digit_three = inputs
    (w, t, e, first, mid, last, turned, left, g, gl, gm, glast, flat, sided, gf) = rest[:15]
    (r0, s1, r1a, r1b, s2a, s2b, r2a, r2b, s3a, s3b, r3a, r3b, rt0, re0, st1, rt1, st2, rt2, rt3, g1, g2, g3,
     send, recv) = rest[15:]
    loads = [pltpu.make_async_copy(sources[i], inputs[i], sems.at[i]) for i in range(12)]
    for i in (9, 11, 10, 0, 2, 1, 8, 3, 4, 5, 6, 7):
        loads[i].start()
    core, x, u, v = whereabouts()
    y = (1 - core) * u + core * v
    z = core * u + (1 - core) * v
    mate = ((z // 2) * 8 + x * 2 + (1 - core), (z % 2) * 8 + y)
    other_x = {k: place(core, (x + k) % 4, u, v) for k in XORDER}
    other_u = {k: place(core, x, (u + k) % 8, v) for k in ORDER}
    other_v = {k: place(core, x, u, (v + k) % 8) for k in ORDER}
    barrier = pltpu.get_barrier_semaphore()
    peers = [mate] + list(other_x.values()) + list(other_u.values()) + list(other_v.values())
    for peer in peers:
        pl.semaphore_signal(barrier, inc=1, device_id=peer, device_id_type=MESH)
    copies = []

    def put(src, dst, peer):
        spot = len(copies)
        copy = pltpu.make_async_remote_copy(
            src_ref=src, dst_ref=dst, send_sem=send.at[spot], recv_sem=recv.at[spot],
            device_id=peer, device_id_type=MESH)
        copy.start()
        copies.append(copy)
        return copy

    def arrived(group):
        for copy in group:
            copy.wait_recv()

    for load in loads:
        load.wait()

    bf16, f32 = jnp.bfloat16, jnp.float32
    high = lax.Precision.HIGHEST

    def hot(row, count, kind):
        return (lax.broadcasted_iota(jnp.int32, (count, row.shape[1]), 0) == row).astype(kind)

    hot_one = hot(digit_one[...], 200, bf16)
    hot_two = hot(digit_two[...], 200, bf16)
    hot_three = hot(digit_three[...], 250, bf16)
    bag = hot(bags[...], 64, f32)
    first[...] = contract(one[...], hot_one, 0, 0)
    ends = contract(three[...], hot_three, 0, 0)
    last[...] = ends
    for side in range(2):
        sided[side] = ends[:, side * 128:side * 128 + 128]
        for d in range(8):
            turned[d * 32:d * 32 + 32, side * 128:side * 128 + 128] = sided.at[side][pl.ds(d, 32, stride=8), :]
    for part in range(8):
        mid[part * 512:part * 512 + 512, :] = contract(two[:, part * 512:part * 512 + 512], hot_two, 0, 0)

    for b in range(4):
        sums = [jnp.zeros((32, 256), f32) for _ in range(4)]
        for a in range(32):
            piece = mid[a * 128 + b * 32:a * 128 + b * 32 + 32, :]
            sums = [total + first[i * 32 + a:i * 32 + a + 1, :] * piece for i, total in enumerate(sums)]
        for i in range(4):
            left[(i * 4 + b) * 32:(i * 4 + b) * 32 + 32, :] = sums[i]
    rows = []
    for p in range(16):
        total = jnp.zeros((8, 256), f32)
        for a in range(32):
            total = total + left[p * 32 + a:p * 32 + a + 1, :] * last[a * 8:a * 8 + 8, :]
        rows.append(total)
    embedded = jnp.concatenate(rows, axis=0)

    pooled = contract(bag, embedded, 1, 1, precision=high)
    joined = jnp.concatenate([dense[...], pooled.astype(bf16)], axis=1)
    pre = jnp.dot(joined, w_top[...], preferred_element_type=f32) + bias[...]
    sig = jax.nn.sigmoid(pre)
    hidden = pre * sig
    logit = jnp.sum(hidden * w_out[...], axis=1, keepdims=True)
    square = lax.broadcasted_iota(jnp.int32, (64, 64), 0) == lax.broadcasted_iota(jnp.int32, (64, 64), 1)
    label = jnp.sum(jnp.where(square, labels[...].astype(f32), 0.0), axis=1, keepdims=True)
    dlogit = (jax.nn.sigmoid(logit) - label) / 64
    dpre = dlogit * w_out[...] * (sig * (1.0 + pre * (1.0 - sig)))
    low = dpre.astype(bf16)
    weight = contract(joined, low, 0, 0)
    t[0] = weight[:, 0:128]
    t[1] = weight[:, 128:256]
    grad_bias = jnp.sum(dpre, axis=0, keepdims=True)
    grad_out = jnp.sum(hidden * dlogit, axis=0, keepdims=True)
    e[...] = jnp.concatenate([grad_bias[:, :128], grad_bias[:, 128:], grad_out[:, :128], grad_out[:, 128:],
                              jnp.zeros((4, 128), f32)], axis=0)
    pooled_grad = contract(w_top[128:256, :], low, 1, 1)
    g[...] = jnp.dot(pooled_grad, bag, precision=high, preferred_element_type=f32)

    pl.semaphore_wait(barrier, len(peers))
    t0 = [put(t.at[1 - core], rt0, mate), put(e, re0, mate)]

    for a in range(32):
        total = jnp.zeros((8, 256), f32)
        for p in range(16):
            total = total + left[p * 32 + a:p * 32 + a + 1, :] * g[p * 8:p * 8 + 8, :]
        glast[a * 8:a * 8 + 8, :] = total
    for p in range(16):
        total = jnp.zeros((32, 256), f32)
        for d in range(8):
            total = total + g[p * 8 + d:p * 8 + d + 1, :] * turned[d * 32:d * 32 + 32, :]
        gl[p * 32:p * 32 + 32, :] = total

    def scatter(table, value):
        upper, lower = halves(value)
        return contract(table, upper, 1, 1) + contract(table, lower, 1, 1)

    for a in range(0, 32, 2):
        for half in range(2):
            c = a + half
            partial = [jnp.zeros((8, 256), f32) for _ in range(4)]
            for b in range(16):
                piece = mid[c * 128 + b * 8:c * 128 + b * 8 + 8, :]
                total = jnp.zeros((8, 256), f32)
                for i in range(4):
                    slope = gl[i * 128 + b * 8:i * 128 + b * 8 + 8, :]
                    total = total + first[i * 32 + c:i * 32 + c + 1, :] * slope
                    partial[i] = partial[i] + slope * piece
                gm[half * 128 + b * 8:half * 128 + b * 8 + 8, :] = total
            for i in range(4):
                for side in range(2):
                    gf.at[side][pl.ds(i * 32 + c, 8, stride=128), :] = partial[i][:, side * 128:side * 128 + 128]
        middle = scatter(hot_two, gm[...])
        flat[pl.ds(200 + a, 200, stride=32), :] = middle[:, 0:128]
        flat[pl.ds(201 + a, 200, stride=32), :] = middle[:, 128:256]
    spread = scatter(hot_one, jnp.concatenate([gf[0], gf[1]], axis=1))
    total = spread[:, 0:128]
    for part in range(1, 8):
        total = total + spread[:, part * 128:part * 128 + 128]
    flat[7096:7104, :] = jnp.zeros((8, 128), f32)
    flat[0:200, :] = total
    ending = scatter(hot_three, glast[...])
    flat[pl.ds(6600, 250, stride=2), :] = ending[:, 0:128]
    flat[pl.ds(6601, 250, stride=2), :] = ending[:, 128:256]

    for q in range(512):
        side, qx, qy = (q // 16) % 2, (q // 32) % 4, q % 8
        qz = (q // 128) * 2 + (q // 8) % 2
        qu, qv = (qy, qz) if side == 0 else (qz, qy)
        start, upper_at, lower_at = (1775 * q) // 128, (qx * 64 + qu * 8 + qv) * 8, (qu * 32 + qv * 4 + qx) * 8
        w[side, 0, upper_at:upper_at + 8, :] = flat[start:start + 8, :]
        w[side, 1, lower_at:lower_at + 8, :] = flat[start + 8:start + 16, :]

    p0 = [put(w.at[1 - core, color], r0.at[color], mate) for color in (0, 1)]
    arrived(t0)
    extra = e[...] + re0[...]
    for part in range(4):
        rows = pl.ds(part * 64, 64)
        st1[part, 0:64, :] = t[core, rows, :] + rt0[rows, :]
        st1[part, 64:72, :] = extra
    t1 = [put(st1.at[(x + k) % 4], rt1.at[x], other_x[k]) for k in XORDER]
    rt1[x] = st1[x]


    def fold(color):
        def store(at, value):
            s1[color, at, :] = value
        summed(2048, 256, store, lambda at: w[core, color, at, :], lambda at: r0[color, at, :])

    arrived(p0[:1])
    fold(0)
    p1a = [put(s1.at[0, pl.ds(((x + k) % 4) * 512, 512)], r1a.at[k - 1], other_x[k]) for k in XORDER]
    arrived(p0[1:])
    fold(1)
    p1b = [put(s1.at[1, pl.ds(((u + k) % 8) * 256, 256)], r1b.at[k - 1], other_u[k]) for k in ORDER]

    arrived(t1)
    total = rt1[0]
    for part in range(1, 4):
        total = total + rt1[part]
    for part in range(8):
        st2[part, 0:8, :] = total[part * 8:part * 8 + 8]
        st2[part, 8:16, :] = total[64:72]
    t2 = [put(st2.at[(v + k) % 8], rt2.at[v], other_v[k]) for k in ORDER]
    rt2[v] = st2[v]
    arrived(t2)
    total = rt2[0]
    for part in range(1, 8):
        total = total + rt2[part]
    rt3[u] = total
    t3 = [put(rt3.at[u], rt3.at[u], other_u[k]) for k in ORDER]

    arrived(p1a)

    def store2a(at, value):
        s2a[at, :] = value

    summed(512, 128, store2a, lambda at: s1[0, pl.ds(x * 512 + at.start, at.size), :],
           *[functools.partial(lambda k, at: r1a[k, at, :], k) for k in range(3)])
    p2a = [put(s2a.at[pl.ds(((u + k) % 8) * 64, 64)], r2a.at[k - 1], other_u[k]) for k in ORDER]
    arrived(p1b)

    def store2b(at, value):
        s2b[at, :] = value

    summed(256, 64, store2b, lambda at: s1[1, pl.ds(u * 256 + at.start, at.size), :],
           *[functools.partial(lambda k, at: r1b[k, at, :], k) for k in range(7)])
    p2b = [put(s2b.at[pl.ds(((v + k) % 8) * 32, 32)], r2b.at[k - 1], other_v[k]) for k in ORDER]

    arrived(t3)
    total = rt3[0]
    for part in range(1, 8):
        total = total + rt3[part]
    g1[v] = total[0:8]
    extra = total[8:16]
    t4 = [put(g1.at[v], g1.at[v], other_v[k]) for k in ORDER]

    arrived(p2a)
    total = s2a[pl.ds(u * 64, 64), :]
    for part in range(7):
        total = total + r2a[part]
    s3a[...] = total
    p3a = [put(s3a.at[pl.ds(((v + k) % 8) * 8, 8)], r3a.at[k - 1], other_v[k]) for k in ORDER]
    arrived(p2b)
    total = s2b[pl.ds(v * 32, 32), :]
    for part in range(7):
        total = total + r2b[part]
    s3b[...] = total
    p3b = [put(s3b.at[pl.ds(((x + k) % 4) * 8, 8)], r3b.at[k - 1], other_x[k]) for k in XORDER]

    arrived(t4)
    g2[x] = g1[...]
    t5 = [put(g2.at[x], g2.at[x], other_x[k]) for k in XORDER]
    for copy in t5:
        copy.wait_recv()
    t6 = put(g2, g3, mate)

    arrived(p3a)
    upper = s3a[pl.ds(v * 8, 8), :]
    for part in range(7):
        upper = upper + r3a[part]
    arrived(p3b)
    lower = s3b[pl.ds(x * 8, 8), :]
    for part in range(3):
        lower = lower + r3b[part]
    gx, gy = lax.axis_index("gx"), lax.axis_index("gy")
    offset = ((gx * 16 + gy) * 1775) % 128
    turned = pltpu.roll(jnp.concatenate([upper, lower], axis=0), (128 - offset) % 128, 1)
    below = pltpu.roll(turned, 15, 0)
    lane = lax.broadcasted_iota(jnp.int32, (16, 128), 1)
    out[...] = jnp.where(lane < 128 - offset, turned, below)

    top[256:257, 0:128] = extra[0:1]
    top[256:257, 128:256] = extra[1:2]
    top[257:258, 0:128] = extra[2:3]
    top[257:258, 128:256] = extra[3:4]
    arrived([t6])

    @pl.when(core == 0)
    def _():
        top[0:256, 0:128] = g2[...].reshape(256, 128)
        top[0:256, 128:256] = g3[...].reshape(256, 128)

    @pl.when(core == 1)
    def _():
        top[0:256, 128:256] = g2[...].reshape(256, 128)
        top[0:256, 0:128] = g3[...].reshape(256, 128)

    for copy in copies:
        copy.wait_send()


def step(*args):
    bf16, f32, i32 = jnp.bfloat16, jnp.float32, jnp.int32
    kinds = [jax.typeof(arg) for arg in args]
    vmem = pl.BlockSpec(memory_space=pltpu.VMEM)
    wide = [128, 4096, 256, 256, 512, 128, 512, 256, 256]
    shapes = [(2, 2048), (2, 2048), (3, 512), (7, 256), (512,), (256,), (7, 64), (7, 32), (64,), (32,), (7, 8), (3, 8),
              (256,), (8,), (4, 72), (4, 72), (8, 16), (8, 16), (8, 16), (8, 8), (4, 8, 8), (4, 8, 8)]
    scratch = [pltpu.VMEM(kind.shape, kind.dtype) for kind in kinds] + [pltpu.SemaphoreType.DMA((12,))]
    scratch += [pltpu.VMEM(shape + (128,), f32) for shape in ((2, 2, 2048), (2, 256), (8,))]
    scratch += [pltpu.VMEM((count, 256), f32) for count in wide]
    scratch += [pltpu.VMEM(shape + (128,), f32) for shape in [(7104,), (2, 256), (2, 1024)] + shapes]
    scratch += [pltpu.SemaphoreType.DMA((70,)), pltpu.SemaphoreType.DMA((70,))]
    return pl.pallas_call(
        step_kernel,
        out_shape=(jax.ShapeDtypeStruct((16, 128), f32), jax.ShapeDtypeStruct((258, 256), f32)),
        in_specs=[pl.BlockSpec(memory_space=pl.ANY)] * 12,
        out_specs=(vmem, vmem),
        scratch_shapes=scratch,
        compiler_params=pltpu.CompilerParams(collective_id=0, has_side_effects=True, vmem_limit_bytes=36 * 1024 * 1024),
        name="step",
    )(*args)


def per_device(core_one, core_two, core_three, dense_rows, w_top, bias_top, w_out, labels, bag_ids, digit_one, digit_two,
               digit_three):
    chunk, top_grad = step(core_one, core_two, core_three, dense_rows, w_top, bias_top[None], w_out[None], labels[None],
                           bag_ids, digit_one, digit_two, digit_three)
    return (chunk.reshape(-1)[:1775], top_grad)


def solution(mesh):
    return jax.shard_map(
        per_device,
        mesh=mesh,
        in_specs=(
            P(),
            P(),
            P(),
            P(("gx", "gy"), None),
            P(),
            P(),
            P(),
            P(("gx", "gy")),
            P(("gx", "gy"), None),
            P(("gx", "gy"), None),
            P(("gx", "gy"), None),
            P(("gx", "gy"), None),
        ),
        out_specs=(P(("gx", "gy")), P()),
        check_vma=False,
    )
```

```python
import functools

import jax
import jax.numpy as jnp
from jax import lax
from jax.experimental import pallas as pl
from jax.experimental.pallas import tpu as pltpu
from jax.sharding import PartitionSpec as P

MESH = pl.DeviceIdType.MESH
ORDER = (1, 7, 2, 6, 3, 5, 4)
XORDER = (1, 3, 2)


def whereabouts():
    gx, gy = lax.axis_index("gx"), lax.axis_index("gy")
    core, x = gx % 2, (gx // 2) % 4
    y, z = gy % 8, (gx // 8) * 2 + gy // 8
    u = (1 - core) * y + core * z
    v = (1 - core) * z + core * y
    return core, x, u, v


def place(core, x, u, v):
    y = (1 - core) * u + core * v
    z = core * u + (1 - core) * v
    return ((z // 2) * 8 + x * 2 + core, (z % 2) * 8 + y)


def summed(rows, step, store, *parts):
    def body(i, carry):
        at = pl.ds(pl.multiple_of(i * step, step), step)
        total = parts[0](at)
        for part in parts[1:]:
            total = total + part(at)
        store(at, total)
        return carry

    lax.fori_loop(0, rows // step, body, 0)


def contract(a, b, left, right, **kw):
    return lax.dot_general(a, b, (((left,), (right,)), ((), ())), preferred_element_type=jnp.float32, **kw)


def halves(value):
    high = value.astype(jnp.bfloat16)
    return high, (value - high.astype(jnp.float32)).astype(jnp.bfloat16)


def step_kernel(*refs):
    sources, (out, top), rest = refs[:12], refs[12:14], refs[14:]
    inputs, sems, rest = rest[:12], rest[12], rest[13:]
    one, two, three, dense, w_top, bias, w_out, labels, bags, digit_one, digit_two, digit_three = inputs
    (w, t, e, first, mid, last, turned, left, g, gl, gm, glast, flat, sided, gf) = rest[:15]
    (r0, s1, r1a, r1b, s2a, s2b, r2a, r2b, s3a, s3b, r3a, r3b, rt0, re0, st1, rt1, st2, rt2, rt3, g1, g2, g3, rel_a, rel_b,
     send, recv) = rest[15:]
    loads = [pltpu.make_async_copy(sources[i], inputs[i], sems.at[i]) for i in range(12)]
    for i in (9, 11, 10, 0, 2, 1, 8, 3, 4, 5, 6, 7):
        loads[i].start()
    core, x, u, v = whereabouts()
    y = (1 - core) * u + core * v
    z = core * u + (1 - core) * v
    mate = ((z // 2) * 8 + x * 2 + (1 - core), (z % 2) * 8 + y)
    other_x = {k: place(core, (x + k) % 4, u, v) for k in XORDER}
    other_u = {k: place(core, x, (u + k) % 8, v) for k in ORDER}
    other_v = {k: place(core, x, u, (v + k) % 8) for k in ORDER}
    barrier = pltpu.get_barrier_semaphore()
    peers = [mate] + list(other_x.values()) + list(other_u.values()) + list(other_v.values())
    for peer in peers:
        pl.semaphore_signal(barrier, inc=1, device_id=peer, device_id_type=MESH)
    copies = []

    def put(src, dst, peer):
        spot = len(copies)
        copy = pltpu.make_async_remote_copy(
            src_ref=src, dst_ref=dst, send_sem=send.at[spot], recv_sem=recv.at[spot],
            device_id=peer, device_id_type=MESH)
        copy.start()
        copies.append(copy)
        return copy

    def arrived(group):
        for copy in group:
            copy.wait_recv()

    for i in (9, 0, 11, 2, 10, 8):
        loads[i].wait()
    bf16, f32 = jnp.bfloat16, jnp.float32
    high = lax.Precision.HIGHEST

    def hot(row, count, kind):
        return (lax.broadcasted_iota(jnp.int32, (count, row.shape[1]), 0) == row).astype(kind)

    hot_one = hot(digit_one[...], 200, bf16)
    first[...] = contract(one[...], hot_one, 0, 0)
    hot_three = hot(digit_three[...], 250, bf16)
    ends = contract(three[...], hot_three, 0, 0)
    last[...] = ends
    for side in range(2):
        sided[side] = ends[:, side * 128:side * 128 + 128]
        for d in range(8):
            turned[d * 32:d * 32 + 32, side * 128:side * 128 + 128] = sided.at[side][pl.ds(d, 32, stride=8), :]
    hot_two = hot(digit_two[...], 200, bf16)
    bag = hot(bags[...], 64, f32)
    loads[1].wait()
    for part in range(8):
        mid[part * 512:part * 512 + 512, :] = contract(two[:, part * 512:part * 512 + 512], hot_two, 0, 0)

    for b in range(4):
        sums = [jnp.zeros((32, 256), f32) for _ in range(4)]
        for a in range(32):
            piece = mid[a * 128 + b * 32:a * 128 + b * 32 + 32, :]
            sums = [total + first[i * 32 + a:i * 32 + a + 1, :] * piece for i, total in enumerate(sums)]
        for i in range(4):
            left[(i * 4 + b) * 32:(i * 4 + b) * 32 + 32, :] = sums[i]
    rows = []
    for p in range(16):
        total = jnp.zeros((8, 256), f32)
        for a in range(32):
            total = total + left[p * 32 + a:p * 32 + a + 1, :] * last[a * 8:a * 8 + 8, :]
        rows.append(total)
    embedded = jnp.concatenate(rows, axis=0)

    for i in (3, 4, 5, 6, 7):
        loads[i].wait()
    pooled = contract(bag, embedded, 1, 1, precision=high)
    joined = jnp.concatenate([dense[...], pooled.astype(bf16)], axis=1)
    pre = jnp.dot(joined, w_top[...], preferred_element_type=f32) + bias[...]
    sig = jax.nn.sigmoid(pre)
    hidden = pre * sig
    logit = jnp.sum(hidden * w_out[...], axis=1, keepdims=True)
    square = lax.broadcasted_iota(jnp.int32, (64, 64), 0) == lax.broadcasted_iota(jnp.int32, (64, 64), 1)
    label = jnp.sum(jnp.where(square, labels[...].astype(f32), 0.0), axis=1, keepdims=True)
    dlogit = (jax.nn.sigmoid(logit) - label) / 64
    dpre = dlogit * w_out[...] * (sig * (1.0 + pre * (1.0 - sig)))
    low = dpre.astype(bf16)
    weight = contract(joined, low, 0, 0)
    t[0] = weight[:, 0:128]
    t[1] = weight[:, 128:256]
    grad_bias = jnp.sum(dpre, axis=0, keepdims=True)
    grad_out = jnp.sum(hidden * dlogit, axis=0, keepdims=True)
    e[...] = jnp.concatenate([grad_bias[:, :128], grad_bias[:, 128:], grad_out[:, :128], grad_out[:, 128:],
                              jnp.zeros((4, 128), f32)], axis=0)
    pooled_grad = contract(w_top[128:256, :], low, 1, 1)
    g[...] = jnp.dot(pooled_grad, bag, precision=high, preferred_element_type=f32)

    pl.semaphore_wait(barrier, len(peers))
    t0 = [put(t.at[1 - core], rt0, mate), put(e, re0, mate)]

    for a in range(32):
        total = jnp.zeros((8, 256), f32)
        for p in range(16):
            total = total + left[p * 32 + a:p * 32 + a + 1, :] * g[p * 8:p * 8 + 8, :]
        glast[a * 8:a * 8 + 8, :] = total
    for p in range(16):
        total = jnp.zeros((32, 256), f32)
        for d in range(8):
            total = total + g[p * 8 + d:p * 8 + d + 1, :] * turned[d * 32:d * 32 + 32, :]
        gl[p * 32:p * 32 + 32, :] = total

    def scatter(table, value):
        upper, lower = halves(value)
        return contract(table, upper, 1, 1) + contract(table, lower, 1, 1)

    def middles(low_a, high_a):
        for a in range(low_a, high_a, 2):
            for c in (a, a + 1):
                partial = [jnp.zeros((8, 256), f32) for _ in range(4)]
                scale = [jnp.broadcast_to(first[i * 32 + c:i * 32 + c + 1, :], (8, 256)) for i in range(4)]
                for b in range(8):
                    totals = []
                    for at in (c * 128 + b * 16, c * 128 + b * 16 + 8):
                        piece = mid[at:at + 8, :]
                        total = None
                        for i in range(4):
                            low_at = i * 128 + at - c * 128
                            slope = gl[low_at:low_at + 8, :]
                            total = scale[i] * slope if total is None else total + scale[i] * slope
                            partial[i] = partial[i] + slope * piece
                        totals.append(total)
                    gm[c * 128 + b * 16:c * 128 + b * 16 + 16, :] = jnp.concatenate(totals, axis=0).astype(bf16)
                for i in range(4):
                    for side in range(2):
                        gf.at[side][pl.ds(i * 32 + c, 8, stride=128), :] = partial[i][:, side * 128:side * 128 + 128]
            middle = contract(hot_two, gm[a * 128:a * 128 + 256, :], 1, 1)
            flat[pl.ds(200 + a, 200, stride=32), :] = middle[:, 0:128]
            flat[pl.ds(201 + a, 200, stride=32), :] = middle[:, 128:256]

    arrived(t0)
    extra = e[...] + re0[...]
    for part in range(4):
        rows = pl.ds(part * 64, 64)
        st1[part, 0:64, :] = t[core, rows, :] + rt0[rows, :]
        st1[part, 64:72, :] = extra
    t1 = [put(st1.at[(x + k) % 4], rt1.at[x], other_x[k]) for k in XORDER]
    rt1[x] = st1[x]

    middles(0, 16)
    arrived(t1)
    total = rt1[0]
    for part in range(1, 4):
        total = total + rt1[part]
    for part in range(8):
        st2[part, 0:8, :] = total[part * 8:part * 8 + 8]
        st2[part, 8:16, :] = total[64:72]
    t2 = [put(st2.at[(v + k) % 8], rt2.at[v], other_v[k]) for k in ORDER]
    rt2[v] = st2[v]

    middles(16, 32)
    spread = scatter(hot_one, jnp.concatenate([gf[0], gf[1]], axis=1))
    total = spread[:, 0:128]
    for part in range(1, 8):
        total = total + spread[:, part * 128:part * 128 + 128]
    flat[7096:7104, :] = jnp.zeros((8, 128), f32)
    flat[0:200, :] = total
    ending = scatter(hot_three, glast[...])
    flat[pl.ds(6600, 250, stride=2), :] = ending[:, 0:128]
    flat[pl.ds(6601, 250, stride=2), :] = ending[:, 128:256]

    for q in range(512):
        side, qx, qy = (q // 16) % 2, (q // 32) % 4, q % 8
        qz = (q // 128) * 2 + (q // 8) % 2
        qu, qv = (qy, qz) if side == 0 else (qz, qy)
        start, upper_at, lower_at = (1775 * q) // 128, (qx * 64 + qu * 8 + qv) * 8, (qu * 32 + qx * 8 + qv) * 8
        w[side, 0, upper_at:upper_at + 8, :] = flat[start:start + 8, :]
        w[side, 1, lower_at:lower_at + 8, :] = flat[start + 8:start + 16, :]

    p0 = [put(w.at[1 - core, color], r0.at[color], mate) for color in (1, 0)]
    arrived(t2)
    total = rt2[0]
    for part in range(1, 8):
        total = total + rt2[part]
    rt3[u] = total
    t3 = [put(rt3.at[u], rt3.at[u], other_u[k]) for k in ORDER]

    def fold(color):
        def store(at, value):
            s1[color, at, :] = value
        summed(2048, 256, store, lambda at: w[core, color, at, :], lambda at: r0[color, at, :])

    def part1(color, slot, rows, half=None):
        size = rows if half is None else rows // 2
        return s1.at[color, pl.ds(slot * rows + (0 if half is None else half * size), size)]

    def relayed(color, slot, rows, half, came):
        at = pl.ds(slot * rows + half * (rows // 2), rows // 2)
        s1[color, at, :] = s1[color, at, :] + came[...]

    arrived(p0[:1])
    fold(1)
    far = (u + 4) % 8
    relay_b = [put(part1(1, far, 256, 0), rel_b.at[0], other_u[2]), put(part1(1, far, 256, 1), rel_b.at[1], other_u[6])]
    p1b = [put(part1(1, (u + k) % 8, 256), r1b.at[k - 1], other_u[k]) for k in (3, 5)]
    p1b += [put(part1(1, (u + 2) % 8, 256, 1), r1b.at[1, pl.ds(128, 128)], other_u[2]),
            put(part1(1, (u + 6) % 8, 256, 0), r1b.at[5, pl.ds(0, 128)], other_u[6])]
    p1b += [put(part1(1, (u + k) % 8, 256), r1b.at[k - 1], other_u[k]) for k in (1, 7)]
    arrived(p0[1:])
    fold(0)
    across = (x + 2) % 4
    relay_a = [put(part1(0, across, 512, 0), rel_a.at[0], other_x[1]), put(part1(0, across, 512, 1), rel_a.at[1], other_x[3])]
    p1a = [put(part1(0, (x + 1) % 4, 512, 1), r1a.at[0, pl.ds(256, 256)], other_x[1]),
           put(part1(0, (x + 3) % 4, 512, 0), r1a.at[1, pl.ds(0, 256)], other_x[3])]
    arrived(relay_b)
    relayed(1, (u + 2) % 8, 256, 0, rel_b.at[0])
    relayed(1, (u + 6) % 8, 256, 1, rel_b.at[1])
    p1b += [put(part1(1, (u + 2) % 8, 256, 0), r1b.at[1, pl.ds(0, 128)], other_u[2]),
            put(part1(1, (u + 6) % 8, 256, 1), r1b.at[5, pl.ds(128, 128)], other_u[6])]
    arrived(relay_a)
    relayed(0, (x + 1) % 4, 512, 0, rel_a.at[0])
    relayed(0, (x + 3) % 4, 512, 1, rel_a.at[1])
    p1a += [put(part1(0, (x + 1) % 4, 512, 0), r1a.at[0, pl.ds(0, 256)], other_x[1]),
            put(part1(0, (x + 3) % 4, 512, 1), r1a.at[1, pl.ds(256, 256)], other_x[3])]

    arrived(t3)
    total = rt3[0]
    for part in range(1, 8):
        total = total + rt3[part]
    g1[v] = total[0:8]
    extra = total[8:16]
    t4 = [put(g1.at[v], g1.at[v], other_v[k]) for k in ORDER]

    arrived(p1a)

    def store2a(at, value):
        s2a[at, :] = value

    summed(512, 128, store2a, lambda at: s1[0, pl.ds(x * 512 + at.start, at.size), :],
           *[functools.partial(lambda k, at: r1a[k, at, :], k) for k in range(2)])
    p2a = [put(s2a.at[pl.ds(((u + k) % 8) * 64, 64)], r2a.at[k - 1], other_u[k]) for k in ORDER]
    arrived(t4)
    g2[x] = g1[...]
    t5 = [put(g2.at[x], g2.at[x], other_x[k]) for k in XORDER]
    arrived(p1b)

    def store2b(at, value):
        s2b[at, :] = value

    summed(256, 64, store2b, lambda at: s1[1, pl.ds(u * 256 + at.start, at.size), :],
           *[functools.partial(lambda k, at: r1b[k, at, :], k) for k in (0, 1, 2, 4, 5, 6)])
    p2b = [put(s2b.at[pl.ds(((x + k) % 4) * 64, 64)], r2b.at[k - 1], other_x[k]) for k in XORDER]
    arrived(p2b)
    total = s2b[pl.ds(x * 64, 64), :]
    for part in range(3):
        total = total + r2b[part]
    s3b[...] = total
    p3b = [put(s3b.at[pl.ds(((v + k) % 8) * 8, 8)], r3b.at[k - 1], other_v[k]) for k in ORDER]
    arrived(p2a)
    total = s2a[pl.ds(u * 64, 64), :]
    for part in range(7):
        total = total + r2a[part]
    s3a[...] = total
    p3a = [put(s3a.at[pl.ds(((v + k) % 8) * 8, 8)], r3a.at[k - 1], other_v[k]) for k in ORDER]

    arrived(t5)
    t6 = put(g2, g3, mate)
    arrived(p3b)
    lower = s3b[pl.ds(v * 8, 8), :]
    for part in range(7):
        lower = lower + r3b[part]
    arrived(p3a)
    upper = s3a[pl.ds(v * 8, 8), :]
    for part in range(7):
        upper = upper + r3a[part]
    gx, gy = lax.axis_index("gx"), lax.axis_index("gy")
    offset = ((gx * 16 + gy) * 1775) % 128
    turned = pltpu.roll(jnp.concatenate([upper, lower], axis=0), (128 - offset) % 128, 1)
    below = pltpu.roll(turned, 15, 0)
    lane = lax.broadcasted_iota(jnp.int32, (16, 128), 1)
    out[...] = jnp.where(lane < 128 - offset, turned, below)

    top[256:257, 0:128] = extra[0:1]
    top[256:257, 128:256] = extra[1:2]
    top[257:258, 0:128] = extra[2:3]
    top[257:258, 128:256] = extra[3:4]
    arrived([t6])

    @pl.when(core == 0)
    def _():
        top[0:256, 0:128] = g2[...].reshape(256, 128)
        top[0:256, 128:256] = g3[...].reshape(256, 128)

    @pl.when(core == 1)
    def _():
        top[0:256, 128:256] = g2[...].reshape(256, 128)
        top[0:256, 0:128] = g3[...].reshape(256, 128)

    for copy in copies:
        copy.wait_send()


def step(*args):
    bf16, f32, i32 = jnp.bfloat16, jnp.float32, jnp.int32
    kinds = [jax.typeof(arg) for arg in args]
    vmem = pl.BlockSpec(memory_space=pltpu.VMEM)
    wide = [128, 4096, 256, 256, 512, 128, 512, 4096, 256]
    shapes = [(2, 2048), (2, 2048), (2, 512), (7, 256), (512,), (256,), (7, 64), (3, 64), (64,), (64,), (7, 8), (7, 8),
              (256,), (8,), (4, 72), (4, 72), (8, 16), (8, 16), (8, 16), (8, 8), (4, 8, 8), (4, 8, 8), (2, 256), (2, 128)]
    scratch = [pltpu.VMEM(kind.shape, kind.dtype) for kind in kinds] + [pltpu.SemaphoreType.DMA((12,))]
    scratch += [pltpu.VMEM(shape + (128,), f32) for shape in ((2, 2, 2048), (2, 256), (8,))]
    scratch += [pltpu.VMEM((count, 256), bf16 if spot == 7 else f32) for spot, count in enumerate(wide)]
    scratch += [pltpu.VMEM(shape + (128,), f32) for shape in [(7104,), (2, 256), (2, 1024)] + shapes]
    scratch += [pltpu.SemaphoreType.DMA((80,)), pltpu.SemaphoreType.DMA((80,))]
    return pl.pallas_call(
        step_kernel,
        out_shape=(jax.ShapeDtypeStruct((16, 128), f32), jax.ShapeDtypeStruct((258, 256), f32)),
        in_specs=[pl.BlockSpec(memory_space=pl.ANY)] * 12,
        out_specs=(vmem, vmem),
        scratch_shapes=scratch,
        compiler_params=pltpu.CompilerParams(collective_id=0, has_side_effects=True, vmem_limit_bytes=58 * 1024 * 1024),
        name="step",
    )(*args)


def per_device(core_one, core_two, core_three, dense_rows, w_top, bias_top, w_out, labels, bag_ids, digit_one, digit_two,
               digit_three):
    chunk, top_grad = step(core_one, core_two, core_three, dense_rows, w_top, bias_top[None], w_out[None], labels[None],
                           bag_ids, digit_one, digit_two, digit_three)
    return (chunk.reshape(-1)[:1775], top_grad)


def solution(mesh):
    return jax.shard_map(
        per_device,
        mesh=mesh,
        in_specs=(
            P(),
            P(),
            P(),
            P(("gx", "gy"), None),
            P(),
            P(),
            P(),
            P(("gx", "gy")),
            P(("gx", "gy"), None),
            P(("gx", "gy"), None),
            P(("gx", "gy"), None),
            P(("gx", "gy"), None),
        ),
        out_specs=(P(("gx", "gy")), P()),
        check_vma=False,
    )
```

```python
import functools

import jax
import jax.numpy as jnp
from jax import lax
from jax.experimental import pallas as pl
from jax.experimental.pallas import tpu as pltpu
from jax.sharding import PartitionSpec as P

MESH = pl.DeviceIdType.MESH
ORDER = (1, 7, 2, 6, 3, 5, 4)
XORDER = (1, 3, 2)


def whereabouts():
    gx, gy = lax.axis_index("gx"), lax.axis_index("gy")
    core, x = gx % 2, (gx // 2) % 4
    y, z = gy % 8, (gx // 8) * 2 + gy // 8
    u = (1 - core) * y + core * z
    v = (1 - core) * z + core * y
    return core, x, u, v


def place(core, x, u, v):
    y = (1 - core) * u + core * v
    z = core * u + (1 - core) * v
    return ((z // 2) * 8 + x * 2 + core, (z % 2) * 8 + y)


def summed(rows, step, store, *parts):
    def body(i, carry):
        at = pl.ds(pl.multiple_of(i * step, step), step)
        total = parts[0](at)
        for part in parts[1:]:
            total = total + part(at)
        store(at, total)
        return carry

    lax.fori_loop(0, rows // step, body, 0)


def contract(a, b, left, right, **kw):
    return lax.dot_general(a, b, (((left,), (right,)), ((), ())), preferred_element_type=jnp.float32, **kw)


def halves(value):
    high = value.astype(jnp.bfloat16)
    return high, (value - high.astype(jnp.float32)).astype(jnp.bfloat16)


def step_kernel(*refs):
    sources, (out, top), rest = refs[:12], refs[12:14], refs[14:]
    inputs, sems, rest = rest[:12], rest[12], rest[13:]
    one, two, three, dense, w_top, bias, w_out, labels, bags, digit_one, digit_two, digit_three = inputs
    (wa, wb, t, e, first, mid, last, turned, left, g, gl, gm, glast, flat, sided, gf) = rest[:16]
    (r0a, r0b, s1a, s1b, r1a, r1b, s2a, s2b, r2a, r2b, s3a, s3b, r3a, r3b, rt0, re0, st1, rt1, st2, rt2, rt3, g1, g2, g3, rel_a, rel_b,
     send, recv) = rest[16:]
    loads = [pltpu.make_async_copy(sources[i], inputs[i], sems.at[i]) for i in range(12)]
    for i in (9, 11, 10, 0, 2, 1, 8, 3, 4, 5, 6, 7):
        loads[i].start()
    core, x, u, v = whereabouts()
    y = (1 - core) * u + core * v
    z = core * u + (1 - core) * v
    mate = ((z // 2) * 8 + x * 2 + (1 - core), (z % 2) * 8 + y)
    other_x = {k: place(core, (x + k) % 4, u, v) for k in XORDER}
    other_u = {k: place(core, x, (u + k) % 8, v) for k in ORDER}
    other_v = {k: place(core, x, u, (v + k) % 8) for k in ORDER}
    barrier = pltpu.get_barrier_semaphore()
    peers = [mate] + list(other_x.values()) + list(other_u.values()) + list(other_v.values())
    for peer in peers:
        pl.semaphore_signal(barrier, inc=1, device_id=peer, device_id_type=MESH)
    copies = []

    def put(src, dst, peer):
        spot = len(copies)
        copy = pltpu.make_async_remote_copy(
            src_ref=src, dst_ref=dst, send_sem=send.at[spot], recv_sem=recv.at[spot],
            device_id=peer, device_id_type=MESH)
        copy.start()
        copies.append(copy)
        return copy

    def arrived(group):
        for copy in group:
            copy.wait_recv()

    for i in (9, 0, 11, 2, 10, 8):
        loads[i].wait()
    bf16, f32 = jnp.bfloat16, jnp.float32
    high = lax.Precision.HIGHEST

    def hot(row, count, kind):
        return (lax.broadcasted_iota(jnp.int32, (count, row.shape[1]), 0) == row).astype(kind)

    hot_one = hot(digit_one[...], 200, bf16)
    first[...] = contract(one[...], hot_one, 0, 0)
    hot_three = hot(digit_three[...], 250, bf16)
    ends = contract(three[...], hot_three, 0, 0)
    last[...] = ends
    for side in range(2):
        sided[side] = ends[:, side * 128:side * 128 + 128]
        for d in range(8):
            turned[d * 32:d * 32 + 32, side * 128:side * 128 + 128] = sided.at[side][pl.ds(d, 32, stride=8), :]
    hot_two = hot(digit_two[...], 200, bf16)
    bag = hot(bags[...], 64, f32)
    loads[1].wait()
    for part in range(8):
        mid[part * 512:part * 512 + 512, :] = contract(two[:, part * 512:part * 512 + 512], hot_two, 0, 0)

    for b in range(4):
        sums = [jnp.zeros((32, 256), f32) for _ in range(4)]
        for a in range(32):
            piece = mid[a * 128 + b * 32:a * 128 + b * 32 + 32, :]
            sums = [total + first[i * 32 + a:i * 32 + a + 1, :] * piece for i, total in enumerate(sums)]
        for i in range(4):
            left[(i * 4 + b) * 32:(i * 4 + b) * 32 + 32, :] = sums[i]
    rows = []
    for p in range(16):
        total = jnp.zeros((8, 256), f32)
        for a in range(32):
            total = total + left[p * 32 + a:p * 32 + a + 1, :] * last[a * 8:a * 8 + 8, :]
        rows.append(total)
    embedded = jnp.concatenate(rows, axis=0)

    for i in (3, 4, 5, 6, 7):
        loads[i].wait()
    pooled = contract(bag, embedded, 1, 1, precision=high)
    joined = jnp.concatenate([dense[...], pooled.astype(bf16)], axis=1)
    pre = jnp.dot(joined, w_top[...], preferred_element_type=f32) + bias[...]
    sig = jax.nn.sigmoid(pre)
    hidden = pre * sig
    logit = jnp.sum(hidden * w_out[...], axis=1, keepdims=True)
    square = lax.broadcasted_iota(jnp.int32, (64, 64), 0) == lax.broadcasted_iota(jnp.int32, (64, 64), 1)
    label = jnp.sum(jnp.where(square, labels[...].astype(f32), 0.0), axis=1, keepdims=True)
    dlogit = (jax.nn.sigmoid(logit) - label) / 64
    dpre = dlogit * w_out[...] * (sig * (1.0 + pre * (1.0 - sig)))
    low = dpre.astype(bf16)
    weight = contract(joined, low, 0, 0)
    t[0] = weight[:, 0:128]
    t[1] = weight[:, 128:256]
    grad_bias = jnp.sum(dpre, axis=0, keepdims=True)
    grad_out = jnp.sum(hidden * dlogit, axis=0, keepdims=True)
    e[...] = jnp.concatenate([grad_bias[:, :128], grad_bias[:, 128:], grad_out[:, :128], grad_out[:, 128:],
                              jnp.zeros((4, 128), f32)], axis=0)
    pooled_grad = contract(w_top[128:256, :], low, 1, 1)
    g[...] = jnp.dot(pooled_grad, bag, precision=high, preferred_element_type=f32)

    pl.semaphore_wait(barrier, len(peers))
    t0 = [put(t.at[1 - core], rt0, mate), put(e, re0, mate)]

    for a in range(32):
        total = jnp.zeros((8, 256), f32)
        for p in range(16):
            total = total + left[p * 32 + a:p * 32 + a + 1, :] * g[p * 8:p * 8 + 8, :]
        glast[a * 8:a * 8 + 8, :] = total
    for p in range(16):
        total = jnp.zeros((32, 256), f32)
        for d in range(8):
            total = total + g[p * 8 + d:p * 8 + d + 1, :] * turned[d * 32:d * 32 + 32, :]
        gl[p * 32:p * 32 + 32, :] = total

    def scatter(table, value):
        upper, lower = halves(value)
        return contract(table, upper, 1, 1) + contract(table, lower, 1, 1)

    def middles(low_a, high_a):
        for a in range(low_a, high_a, 2):
            for c in (a, a + 1):
                partial = [jnp.zeros((8, 256), f32) for _ in range(4)]
                scale = [jnp.broadcast_to(first[i * 32 + c:i * 32 + c + 1, :], (8, 256)) for i in range(4)]
                for b in range(8):
                    totals = []
                    for at in (c * 128 + b * 16, c * 128 + b * 16 + 8):
                        piece = mid[at:at + 8, :]
                        total = None
                        for i in range(4):
                            low_at = i * 128 + at - c * 128
                            slope = gl[low_at:low_at + 8, :]
                            total = scale[i] * slope if total is None else total + scale[i] * slope
                            partial[i] = partial[i] + slope * piece
                        totals.append(total)
                    upper, lower = halves(jnp.concatenate(totals, axis=0))
                    gm[0, c * 128 + b * 16:c * 128 + b * 16 + 16, :] = upper
                    gm[1, c * 128 + b * 16:c * 128 + b * 16 + 16, :] = lower
                for i in range(4):
                    for side in range(2):
                        gf.at[side][pl.ds(i * 32 + c, 8, stride=129), :] = partial[i][:, side * 128:side * 128 + 128]
            middle = contract(hot_two, gm[0, a * 128:a * 128 + 256, :], 1, 1)
            middle = middle + contract(hot_two, gm[1, a * 128:a * 128 + 256, :], 1, 1)
            flat[pl.ds(200 + a, 200, stride=33), :] = middle[:, 0:128]
            flat[pl.ds(201 + a, 200, stride=33), :] = middle[:, 128:256]

    middles(0, 16)
    arrived(t0)
    extra = e[...] + re0[...]
    for part in range(4):
        rows = pl.ds(part * 64, 64)
        st1[part, 0:64, :] = t[core, rows, :] + rt0[rows, :]
        st1[part, 64:72, :] = extra
    t1 = [put(st1.at[(x + k) % 4], rt1.at[x], other_x[k]) for k in XORDER]
    rt1[x] = st1[x]

    ending = scatter(hot_three, glast[...])
    flat[pl.ds(6800, 250, stride=2), :] = ending[:, 0:128]
    flat[pl.ds(6801, 250, stride=2), :] = ending[:, 128:256]
    middles(16, 32)
    total = jnp.zeros((200, 128), f32)
    for part in range(0, 8, 2):
        pieces = [gf[side, at * 129:at * 129 + 128, :] for at in (part, part + 1) for side in (0, 1)]
        spread = scatter(hot_one, jnp.concatenate([jnp.concatenate(pieces[:2], axis=1), jnp.concatenate(pieces[2:], axis=1)], axis=0))
        total = total + spread[:, 0:128] + spread[:, 128:256]
    flat[0:200, :] = total
    flat[7300:7312, :] = jnp.zeros((12, 128), f32)

    def rows_from(start):
        spans, at = [], start
        while at < start + 8:
            if at < 200:
                size, place_at = min(200 - at, start + 8 - at), at
            elif at < 6600:
                size, place_at = min(32 - (at - 200) % 32, start + 8 - at), 200 + (at - 200) // 32 * 33 + (at - 200) % 32
            else:
                size, place_at = start + 8 - at, at + 200
            spans.append((at - start, size, place_at))
            at += size
        return spans

    for q in range(512):
        side, qx, qy = (q // 16) % 2, (q // 32) % 4, q % 8
        qz = (q // 128) * 2 + (q // 8) % 2
        qu, qv = (qy, qz) if side == 0 else (qz, qy)
        for color, slot in ((0, qx * 64 + qu * 8 + qv), (1, qu * 32 + qx * 8 + qv)):
            for shift, size, place_at in rows_from((1775 * q) // 128 + 8 * color):
                if color == 0:
                    wa[side, slot * 8 + shift:slot * 8 + shift + size, :] = flat[place_at:place_at + size, :]
                else:
                    wb[side, slot, shift:shift + size, :] = flat[place_at:place_at + size, :]

    plan = ((0, 2), (1, 4), (1, 3), (1, 5), (0, 1), (0, 3), (1, 2), (1, 6), (1, 1), (1, 7), (0, 0), (1, 0))

    def piece_of(color, distance, x_at, u_at):
        return pl.ds(((x_at + distance) % 4) * 512, 512) if color == 0 else pl.ds(((u_at + distance) % 8) * 32, 32)

    p0 = {}
    for color, distance in plan:
        rows = piece_of(color, distance, x, v)
        if color == 0:
            p0[color, distance] = put(wa.at[1 - core, rows], r0a.at[rows], mate)
        else:
            p0[color, distance] = put(wb.at[1 - core, rows, pl.ds(0, 7)], r0b.at[rows, pl.ds(0, 7)], mate)
    arrived(t1)
    total = rt1[0]
    for part in range(1, 4):
        total = total + rt1[part]
    for part in range(8):
        st2[part, 0:8, :] = total[part * 8:part * 8 + 8]
        st2[part, 8:16, :] = total[64:72]
    t2 = [put(st2.at[(v + k) % 8], rt2.at[v], other_v[k]) for k in ORDER]
    rt2[v] = st2[v]

    def fold(color, distance):
        p0[color, distance].wait_recv()
        rows = piece_of(color, distance, x, u)
        if color == 0:
            s1a[rows, :] = wa[core, rows, :] + r0a[rows, :]
        else:
            s1b[rows, 0:7] = wb[core, rows, 0:7] + r0b[rows, 0:7]

    def part_a(slot, half):
        return s1a.at[pl.ds(slot * 512 + half * 256, 256)]

    def part_b(slot, start=0, size=32):
        return s1b.at[pl.ds(slot * 32 + start, size), pl.ds(0, 7)]

    def land_b(k, start=0, size=32):
        return r1b.at[k - 1, pl.ds(start, size), pl.ds(0, 7)]

    def relayed_a(slot, half, came):
        at = pl.ds(slot * 512 + half * 256, 256)
        s1a[at, :] = s1a[at, :] + came[...]

    def relayed_b(slot, half, way):
        at = pl.ds(slot * 32 + half * 16, 16)
        s1b[at, 0:7] = s1b[at, 0:7] + rel_b[way, :, 0:7]

    far, across = (u + 4) % 8, (x + 2) % 4
    fold(0, 2)
    relay_a = [put(part_a(across, 0), rel_a.at[0], other_x[1]), put(part_a(across, 1), rel_a.at[1], other_x[3])]
    fold(1, 4)
    relay_b = [put(part_b(far, 0, 16), rel_b.at[0, :, pl.ds(0, 7)], other_u[2]), put(part_b(far, 16, 16), rel_b.at[1, :, pl.ds(0, 7)], other_u[6])]
    p1a, p1b = [], []
    for k in (3, 5):
        fold(1, k)
        p1b.append(put(part_b((u + k) % 8), land_b(k), other_u[k]))
    fold(0, 1)
    p1a.append(put(part_a((x + 1) % 4, 1), r1a.at[0, pl.ds(256, 256)], other_x[1]))
    fold(0, 3)
    p1a.append(put(part_a((x + 3) % 4, 0), r1a.at[1, pl.ds(0, 256)], other_x[3]))
    fold(1, 2)
    p1b.append(put(part_b((u + 2) % 8, 16, 16), land_b(2, 16, 16), other_u[2]))
    fold(1, 6)
    p1b.append(put(part_b((u + 6) % 8, 0, 16), land_b(6, 0, 16), other_u[6]))
    arrived(t2)
    total = rt2[0]
    for part in range(1, 8):
        total = total + rt2[part]
    rt3[u] = total
    t3 = [put(rt3.at[u], rt3.at[u], other_u[k]) for k in ORDER]
    for k in (1, 7):
        fold(1, k)
        p1b.append(put(part_b((u + k) % 8), land_b(k), other_u[k]))
    fold(0, 0)
    fold(1, 0)
    arrived(relay_b)
    relayed_b((u + 2) % 8, 0, 0)
    relayed_b((u + 6) % 8, 1, 1)
    p1b += [put(part_b((u + 2) % 8, 0, 16), land_b(2, 0, 16), other_u[2]),
            put(part_b((u + 6) % 8, 16, 16), land_b(6, 16, 16), other_u[6])]
    arrived(relay_a)
    relayed_a((x + 1) % 4, 0, rel_a.at[0])
    relayed_a((x + 3) % 4, 1, rel_a.at[1])
    p1a += [put(part_a((x + 1) % 4, 0), r1a.at[0, pl.ds(0, 256)], other_x[1]),
            put(part_a((x + 3) % 4, 1), r1a.at[1, pl.ds(256, 256)], other_x[3])]

    arrived(t3)
    total = rt3[0]
    for part in range(1, 8):
        total = total + rt3[part]
    g1[v] = total[0:8]
    extra = total[8:16]
    t4 = [put(g1.at[v], g1.at[v], other_v[k]) for k in ORDER]

    arrived(p1a)

    def store2a(at, value):
        s2a[at, :] = value

    summed(512, 128, store2a, lambda at: s1a[pl.ds(x * 512 + at.start, at.size), :],
           *[functools.partial(lambda k, at: r1a[k, at, :], k) for k in range(2)])
    p2a = [put(s2a.at[pl.ds(((u + k) % 8) * 64, 64)], r2a.at[k - 1], other_u[k]) for k in ORDER]
    arrived(p1b)

    def fold2(part, carry):
        at = pl.ds(pl.multiple_of(part * 8, 8), 8)
        total = s1b[pl.ds(u * 32 + part * 8, 8), 0:7]
        for k in (1, 2, 3, 5, 6, 7):
            total = total + r1b[k - 1, at, 0:7]
        s2b[at, 0:7] = total
        return carry

    lax.fori_loop(0, 4, fold2, 0)
    p2b = [put(s2b.at[pl.ds(((x + k) % 4) * 8, 8), pl.ds(0, 7)], r2b.at[k - 1, :, pl.ds(0, 7)], other_x[k]) for k in XORDER]
    arrived(p2b)
    total = s2b[pl.ds(x * 8, 8), 0:7]
    for part in range(3):
        total = total + r2b[part, :, 0:7]
    s3b[:, 0:7] = total
    p3b = [put(s3b.at[(v + k) % 8, pl.ds(0, 7)], r3b.at[k - 1, pl.ds(0, 7)], other_v[k]) for k in ORDER]
    arrived(t4)
    g2[x] = g1[...]
    t5 = [put(g2.at[x], g2.at[x], other_x[k]) for k in XORDER]
    arrived(p2a)
    total = s2a[pl.ds(u * 64, 64), :]
    for part in range(7):
        total = total + r2a[part]
    s3a[...] = total
    p3a = [put(s3a.at[pl.ds(((v + k) % 8) * 8, 8)], r3a.at[k - 1], other_v[k]) for k in ORDER]

    arrived(t5)
    t6 = put(g2, g3, mate)
    arrived(p3b)
    lower = s3b[v, 0:7]
    for part in range(7):
        lower = lower + r3b[part, 0:7]
    lower = jnp.concatenate([lower, jnp.zeros((1, 128), f32)], axis=0)
    arrived(p3a)
    upper = s3a[pl.ds(v * 8, 8), :]
    for part in range(7):
        upper = upper + r3a[part]
    gx, gy = lax.axis_index("gx"), lax.axis_index("gy")
    offset = ((gx * 16 + gy) * 1775) % 128
    turned = pltpu.roll(jnp.concatenate([upper, lower], axis=0), (128 - offset) % 128, 1)
    below = pltpu.roll(turned, 15, 0)
    lane = lax.broadcasted_iota(jnp.int32, (16, 128), 1)
    out[...] = jnp.where(lane < 128 - offset, turned, below)

    top[256:257, 0:128] = extra[0:1]
    top[256:257, 128:256] = extra[1:2]
    top[257:258, 0:128] = extra[2:3]
    top[257:258, 128:256] = extra[3:4]
    arrived([t6])

    @pl.when(core == 0)
    def _():
        top[0:256, 0:128] = g2[...].reshape(256, 128)
        top[0:256, 128:256] = g3[...].reshape(256, 128)

    @pl.when(core == 1)
    def _():
        top[0:256, 128:256] = g2[...].reshape(256, 128)
        top[0:256, 0:128] = g3[...].reshape(256, 128)

    for copy in copies:
        copy.wait_send()


def step(*args):
    bf16, f32, i32 = jnp.bfloat16, jnp.float32, jnp.int32
    kinds = [jax.typeof(arg) for arg in args]
    vmem = pl.BlockSpec(memory_space=pltpu.VMEM)
    wide = [128, 4096, 256, 256, 512, 128, 512, None, 256]
    shapes = [(2048,), (256, 8), (2048,), (256, 8), (2, 512), (7, 32, 8), (512,), (32, 8), (7, 64), (3, 8, 8), (64,), (8, 8),
              (7, 8), (7, 8),
              (256,), (8,), (4, 72), (4, 72), (8, 16), (8, 16), (8, 16), (8, 8), (4, 8, 8), (4, 8, 8), (2, 256), (2, 16, 8)]
    scratch = [pltpu.VMEM(kind.shape, kind.dtype) for kind in kinds] + [pltpu.SemaphoreType.DMA((12,))]
    scratch += [pltpu.VMEM(shape + (128,), f32) for shape in ((2, 2048), (2, 256, 8), (2, 256), (8,))]
    scratch += [pltpu.VMEM((count, 256), f32) if count else pltpu.VMEM((2, 4096, 256), bf16) for count in wide]
    scratch += [pltpu.VMEM(shape + (128,), f32) for shape in [(7312,), (2, 256), (2, 1032)] + shapes]
    scratch += [pltpu.SemaphoreType.DMA((90,)), pltpu.SemaphoreType.DMA((90,))]
    return pl.pallas_call(
        step_kernel,
        out_shape=(jax.ShapeDtypeStruct((16, 128), f32), jax.ShapeDtypeStruct((258, 256), f32)),
        in_specs=[pl.BlockSpec(memory_space=pl.ANY)] * 12,
        out_specs=(vmem, vmem),
        scratch_shapes=scratch,
        compiler_params=pltpu.CompilerParams(collective_id=0, has_side_effects=True, vmem_limit_bytes=58 * 1024 * 1024),
        name="step",
    )(*args)


def per_device(core_one, core_two, core_three, dense_rows, w_top, bias_top, w_out, labels, bag_ids, digit_one, digit_two,
               digit_three):
    chunk, top_grad = step(core_one, core_two, core_three, dense_rows, w_top, bias_top[None], w_out[None], labels[None],
                           bag_ids, digit_one, digit_two, digit_three)
    return (chunk.reshape(-1)[:1775], top_grad)


def solution(mesh):
    return jax.shard_map(
        per_device,
        mesh=mesh,
        in_specs=(
            P(),
            P(),
            P(),
            P(("gx", "gy"), None),
            P(),
            P(),
            P(),
            P(("gx", "gy")),
            P(("gx", "gy"), None),
            P(("gx", "gy"), None),
            P(("gx", "gy"), None),
            P(("gx", "gy"), None),
        ),
        out_specs=(P(("gx", "gy")), P()),
        check_vma=False,
    )
```

```python
import functools

import jax
import jax.numpy as jnp
from jax import lax
from jax.experimental import pallas as pl
from jax.experimental.pallas import tpu as pltpu
from jax.sharding import PartitionSpec as P

MESH = pl.DeviceIdType.MESH
ORDER = (1, 7, 2, 6, 3, 5, 4)
XORDER = (1, 3, 2)


def whereabouts():
    gx, gy = lax.axis_index("gx"), lax.axis_index("gy")
    core, x = gx % 2, (gx // 2) % 4
    y, z = gy % 8, (gx // 8) * 2 + gy // 8
    u = (1 - core) * y + core * z
    v = (1 - core) * z + core * y
    return core, x, u, v


def place(core, x, u, v):
    y = (1 - core) * u + core * v
    z = core * u + (1 - core) * v
    return ((z // 2) * 8 + x * 2 + core, (z % 2) * 8 + y)


def summed(rows, step, store, *parts):
    def body(i, carry):
        at = pl.ds(pl.multiple_of(i * step, step), step)
        total = parts[0](at)
        for part in parts[1:]:
            total = total + part(at)
        store(at, total)
        return carry

    lax.fori_loop(0, rows // step, body, 0)


def contract(a, b, left, right, **kw):
    return lax.dot_general(a, b, (((left,), (right,)), ((), ())), preferred_element_type=jnp.float32, **kw)


def halves(value):
    high = value.astype(jnp.bfloat16)
    return high, (value - high.astype(jnp.float32)).astype(jnp.bfloat16)


def step_kernel(*refs):
    sources, (out, top), rest = refs[:12], refs[12:14], refs[14:]
    inputs, sems, rest = rest[:12], rest[12], rest[13:]
    one, two, three, dense, w_top, bias, w_out, labels, bags, digit_one, digit_two, digit_three = inputs
    (wa, wb, t, e, first, mid, last, turned, left, g, gl, gm, glast, flat, sided, gf) = rest[:16]
    (r0a, r0b, s1a, s1b, r1a, r1b, s2a, s2b, r2a, r2b, s3a, s3b, r3a, r3b, rt0, re0, st1, rt1, st2, rt2, rt3, g1, g2, g3, rel_a, rel_b,
     send, recv) = rest[16:]
    loads = [pltpu.make_async_copy(sources[i], inputs[i], sems.at[i]) for i in range(12)]
    for i in (9, 11, 10, 0, 2, 1, 8, 3, 4, 5, 6, 7):
        loads[i].start()
    core, x, u, v = whereabouts()
    y = (1 - core) * u + core * v
    z = core * u + (1 - core) * v
    mate = ((z // 2) * 8 + x * 2 + (1 - core), (z % 2) * 8 + y)
    other_x = {k: place(core, (x + k) % 4, u, v) for k in XORDER}
    other_u = {k: place(core, x, (u + k) % 8, v) for k in ORDER}
    other_v = {k: place(core, x, u, (v + k) % 8) for k in ORDER}
    barrier = pltpu.get_barrier_semaphore()
    peers = [mate] + list(other_x.values()) + list(other_u.values()) + list(other_v.values())
    for peer in peers:
        pl.semaphore_signal(barrier, inc=1, device_id=peer, device_id_type=MESH)
    copies = []

    def put(src, dst, peer):
        spot = len(copies)
        copy = pltpu.make_async_remote_copy(
            src_ref=src, dst_ref=dst, send_sem=send.at[spot], recv_sem=recv.at[spot],
            device_id=peer, device_id_type=MESH)
        copy.start()
        copies.append(copy)
        return copy

    def arrived(group):
        for copy in group:
            copy.wait_recv()

    for i in (9, 0, 11, 2, 10, 8):
        loads[i].wait()
    bf16, f32 = jnp.bfloat16, jnp.float32
    high = lax.Precision.HIGHEST

    def hot(row, count, kind):
        return (lax.broadcasted_iota(jnp.int32, (count, row.shape[1]), 0) == row).astype(kind)

    hot_one = hot(digit_one[...], 200, bf16)
    first[...] = contract(one[...], hot_one, 0, 0)
    hot_three = hot(digit_three[...], 250, bf16)
    ends = contract(three[...], hot_three, 0, 0)
    last[...] = ends
    for side in range(2):
        sided[side] = ends[:, side * 128:side * 128 + 128]
        for d in range(8):
            turned[d * 32:d * 32 + 32, side * 128:side * 128 + 128] = sided.at[side][pl.ds(d, 32, stride=8), :]
    hot_two = hot(digit_two[...], 200, bf16)
    bag = hot(bags[...], 64, f32)
    loads[1].wait()
    for part in range(8):
        mid[part * 512:part * 512 + 512, :] = contract(two[:, part * 512:part * 512 + 512], hot_two, 0, 0)

    for b in range(4):
        sums = [jnp.zeros((32, 256), f32) for _ in range(4)]
        for a in range(32):
            piece = mid[a * 128 + b * 32:a * 128 + b * 32 + 32, :]
            sums = [total + first[i * 32 + a:i * 32 + a + 1, :] * piece for i, total in enumerate(sums)]
        for i in range(4):
            left[(i * 4 + b) * 32:(i * 4 + b) * 32 + 32, :] = sums[i]
    rows = []
    for p in range(16):
        total = jnp.zeros((8, 256), f32)
        for a in range(32):
            total = total + left[p * 32 + a:p * 32 + a + 1, :] * last[a * 8:a * 8 + 8, :]
        rows.append(total)
    embedded = jnp.concatenate(rows, axis=0)

    for i in (3, 4, 5, 6, 7):
        loads[i].wait()
    pooled = contract(bag, embedded, 1, 1, precision=high)
    joined = jnp.concatenate([dense[...], pooled.astype(bf16)], axis=1)
    pre = jnp.dot(joined, w_top[...], preferred_element_type=f32) + bias[...]
    sig = jax.nn.sigmoid(pre)
    hidden = pre * sig
    logit = jnp.sum(hidden * w_out[...], axis=1, keepdims=True)
    square = lax.broadcasted_iota(jnp.int32, (64, 64), 0) == lax.broadcasted_iota(jnp.int32, (64, 64), 1)
    label = jnp.sum(jnp.where(square, labels[...].astype(f32), 0.0), axis=1, keepdims=True)
    dlogit = (jax.nn.sigmoid(logit) - label) / 64
    dpre = dlogit * w_out[...] * (sig * (1.0 + pre * (1.0 - sig)))
    low = dpre.astype(bf16)
    weight = contract(joined, low, 0, 0)
    t[0] = weight[:, 0:128]
    t[1] = weight[:, 128:256]
    grad_bias = jnp.sum(dpre, axis=0, keepdims=True)
    grad_out = jnp.sum(hidden * dlogit, axis=0, keepdims=True)
    e[...] = jnp.concatenate([grad_bias[:, :128], grad_bias[:, 128:], grad_out[:, :128], grad_out[:, 128:],
                              jnp.zeros((4, 128), f32)], axis=0)
    pooled_grad = contract(w_top[128:256, :], low, 1, 1)
    g[...] = jnp.dot(pooled_grad, bag, precision=high, preferred_element_type=f32)

    pl.semaphore_wait(barrier, len(peers))
    t0 = [put(t.at[1 - core], rt0, mate), put(e, re0, mate)]

    for a in range(32):
        total = jnp.zeros((8, 256), f32)
        for p in range(16):
            total = total + left[p * 32 + a:p * 32 + a + 1, :] * g[p * 8:p * 8 + 8, :]
        glast[a * 8:a * 8 + 8, :] = total
    for p in range(16):
        total = jnp.zeros((32, 256), f32)
        for d in range(8):
            total = total + g[p * 8 + d:p * 8 + d + 1, :] * turned[d * 32:d * 32 + 32, :]
        gl[p * 32:p * 32 + 32, :] = total

    def scatter(table, value):
        upper, lower = halves(value)
        return contract(table, upper, 1, 1) + contract(table, lower, 1, 1)

    def middles(low_a, high_a):
        for a in range(low_a, high_a, 2):
            for c in (a, a + 1):
                partial = [jnp.zeros((8, 256), f32) for _ in range(4)]
                scale = [jnp.broadcast_to(first[i * 32 + c:i * 32 + c + 1, :], (8, 256)) for i in range(4)]
                for b in range(8):
                    totals = []
                    for at in (c * 128 + b * 16, c * 128 + b * 16 + 8):
                        piece = mid[at:at + 8, :]
                        total = None
                        for i in range(4):
                            low_at = i * 128 + at - c * 128
                            slope = gl[low_at:low_at + 8, :]
                            total = scale[i] * slope if total is None else total + scale[i] * slope
                            partial[i] = partial[i] + slope * piece
                        totals.append(total)
                    upper, lower = halves(jnp.concatenate(totals, axis=0))
                    gm[0, c * 128 + b * 16:c * 128 + b * 16 + 16, :] = upper
                    gm[1, c * 128 + b * 16:c * 128 + b * 16 + 16, :] = lower
                for i in range(4):
                    for side in range(2):
                        gf.at[side][pl.ds(i * 32 + c, 8, stride=129), :] = partial[i][:, side * 128:side * 128 + 128]
            middle = contract(hot_two, gm[0, a * 128:a * 128 + 256, :], 1, 1)
            middle = middle + contract(hot_two, gm[1, a * 128:a * 128 + 256, :], 1, 1)
            flat[pl.ds(200 + a, 200, stride=33), :] = middle[:, 0:128]
            flat[pl.ds(201 + a, 200, stride=33), :] = middle[:, 128:256]

    middles(0, 16)
    arrived(t0)
    extra = e[...] + re0[...]
    for part in range(4):
        rows = pl.ds(part * 64, 64)
        st1[part, 0:64, :] = t[core, rows, :] + rt0[rows, :]
        st1[part, 64:72, :] = extra
    t1 = [put(st1.at[(x + k) % 4], rt1.at[x], other_x[k]) for k in XORDER]
    rt1[x] = st1[x]

    ending = scatter(hot_three, glast[...])
    flat[pl.ds(6800, 250, stride=2), :] = ending[:, 0:128]
    flat[pl.ds(6801, 250, stride=2), :] = ending[:, 128:256]
    middles(16, 32)
    total = jnp.zeros((200, 128), f32)
    for part in range(0, 8, 2):
        pieces = [gf[side, at * 129:at * 129 + 128, :] for at in (part, part + 1) for side in (0, 1)]
        spread = scatter(hot_one, jnp.concatenate([jnp.concatenate(pieces[:2], axis=1), jnp.concatenate(pieces[2:], axis=1)], axis=0))
        total = total + spread[:, 0:128] + spread[:, 128:256]
    flat[0:200, :] = total
    flat[7300:7312, :] = jnp.zeros((12, 128), f32)

    def rows_from(start):
        spans, at = [], start
        while at < start + 8:
            if at < 200:
                size, place_at = min(200 - at, start + 8 - at), at
            elif at < 6600:
                size, place_at = min(32 - (at - 200) % 32, start + 8 - at), 200 + (at - 200) // 32 * 33 + (at - 200) % 32
            else:
                size, place_at = start + 8 - at, at + 200
            spans.append((at - start, size, place_at))
            at += size
        return spans

    for q in range(512):
        side, qx, qy = (q // 16) % 2, (q // 32) % 4, q % 8
        qz = (q // 128) * 2 + (q // 8) % 2
        qu, qv = (qy, qz) if side == 0 else (qz, qy)
        for color, slot in ((0, qx * 64 + qu * 8 + qv), (1, qu * 32 + qx * 8 + qv)):
            for shift, size, place_at in rows_from((1775 * q) // 128 + 8 * color):
                if color == 0:
                    wa[side, slot * 8 + shift:slot * 8 + shift + size, :] = flat[place_at:place_at + size, :]
                else:
                    wb[side, slot, shift:shift + size, :] = flat[place_at:place_at + size, :]

    plan = ((0, 2), (1, 4), (1, 3), (1, 5), (0, 1), (0, 3), (1, 2), (1, 6), (1, 1), (1, 7), (0, 0), (1, 0))

    def piece_of(color, distance, x_at, u_at):
        return pl.ds(((x_at + distance) % 4) * 512, 512) if color == 0 else pl.ds(((u_at + distance) % 8) * 32, 32)

    p0 = {}
    for color, distance in plan:
        rows = piece_of(color, distance, x, v)
        if color == 0:
            p0[color, distance] = put(wa.at[1 - core, rows], r0a.at[rows], mate)
        else:
            p0[color, distance] = put(wb.at[1 - core, rows, pl.ds(0, 7)], r0b.at[rows, pl.ds(0, 7)], mate)
    arrived(t1)
    total = rt1[0]
    for part in range(1, 4):
        total = total + rt1[part]
    for part in range(8):
        st2[part, 0:8, :] = total[part * 8:part * 8 + 8]
        st2[part, 8:16, :] = total[64:72]
    t2 = [put(st2.at[(v + k) % 8], rt2.at[v], other_v[k]) for k in ORDER]
    rt2[v] = st2[v]

    def fold(color, distance):
        p0[color, distance].wait_recv()
        rows = piece_of(color, distance, x, u)
        if color == 0:
            s1a[rows, :] = wa[core, rows, :] + r0a[rows, :]
        else:
            s1b[rows, 0:7] = wb[core, rows, 0:7] + r0b[rows, 0:7]

    def part_a(slot, half):
        return s1a.at[pl.ds(slot * 512 + half * 256, 256)]

    def part_b(slot, start=0, size=32):
        return s1b.at[pl.ds(slot * 32 + start, size), pl.ds(0, 7)]

    def land_b(k, start=0, size=32):
        return r1b.at[k - 1, pl.ds(start, size), pl.ds(0, 7)]

    def relayed_a(slot, half, came):
        at = pl.ds(slot * 512 + half * 256, 256)
        s1a[at, :] = s1a[at, :] + came[...]

    def relayed_b(slot, half, way):
        at = pl.ds(slot * 32 + half * 16, 16)
        s1b[at, 0:7] = s1b[at, 0:7] + rel_b[way, :, 0:7]

    far, across = (u + 4) % 8, (x + 2) % 4
    fold(0, 2)
    relay_a = [put(part_a(across, 0), rel_a.at[0], other_x[1]), put(part_a(across, 1), rel_a.at[1], other_x[3])]
    fold(1, 4)
    relay_b = [put(part_b(far, 0, 16), rel_b.at[0, :, pl.ds(0, 7)], other_u[2]), put(part_b(far, 16, 16), rel_b.at[1, :, pl.ds(0, 7)], other_u[6])]
    p1a, p1b = [], []
    for k in (3, 5):
        fold(1, k)
        p1b.append(put(part_b((u + k) % 8), land_b(k), other_u[k]))
    fold(0, 1)
    p1a.append(put(part_a((x + 1) % 4, 1), r1a.at[0, pl.ds(256, 256)], other_x[1]))
    fold(0, 3)
    p1a.append(put(part_a((x + 3) % 4, 0), r1a.at[1, pl.ds(0, 256)], other_x[3]))
    fold(1, 2)
    p1b.append(put(part_b((u + 2) % 8, 16, 16), land_b(2, 16, 16), other_u[2]))
    fold(1, 6)
    p1b.append(put(part_b((u + 6) % 8, 0, 16), land_b(6, 0, 16), other_u[6]))
    arrived(t2)
    total = rt2[0]
    for part in range(1, 8):
        total = total + rt2[part]
    rt3[u] = total
    t3 = [put(rt3.at[u], rt3.at[u], other_u[k]) for k in ORDER]
    for k in (1, 7):
        fold(1, k)
        p1b.append(put(part_b((u + k) % 8), land_b(k), other_u[k]))
    fold(0, 0)
    fold(1, 0)
    arrived(relay_b)
    relayed_b((u + 2) % 8, 0, 0)
    relayed_b((u + 6) % 8, 1, 1)
    p1b += [put(part_b((u + 2) % 8, 0, 16), land_b(2, 0, 16), other_u[2]),
            put(part_b((u + 6) % 8, 16, 16), land_b(6, 16, 16), other_u[6])]
    arrived(relay_a)
    relayed_a((x + 1) % 4, 0, rel_a.at[0])
    relayed_a((x + 3) % 4, 1, rel_a.at[1])
    p1a += [put(part_a((x + 1) % 4, 0), r1a.at[0, pl.ds(0, 256)], other_x[1]),
            put(part_a((x + 3) % 4, 1), r1a.at[1, pl.ds(256, 256)], other_x[3])]

    arrived(t3)
    total = rt3[0]
    for part in range(1, 8):
        total = total + rt3[part]
    g1[v] = total[0:8]
    extra = total[8:16]
    t4 = [put(g1.at[v], g1.at[v], other_v[k]) for k in ORDER]

    arrived(p1a)

    def store2a(at, value):
        s2a[at, :] = value

    summed(512, 128, store2a, lambda at: s1a[pl.ds(x * 512 + at.start, at.size), :],
           *[functools.partial(lambda k, at: r1a[k, at, :], k) for k in range(2)])
    p2a = [put(s2a.at[pl.ds(((u + k) % 8) * 64, 64)], r2a.at[k - 1], other_u[k]) for k in ORDER]
    arrived(p1b)

    def fold2(part, carry):
        at = pl.ds(pl.multiple_of(part * 8, 8), 8)
        total = s1b[pl.ds(u * 32 + part * 8, 8), 0:7]
        for k in (1, 2, 3, 5, 6, 7):
            total = total + r1b[k - 1, at, 0:7]
        s2b[at, 0:7] = total
        return carry

    lax.fori_loop(0, 4, fold2, 0)
    p2b = [put(s2b.at[pl.ds(((x + k) % 4) * 8, 8), pl.ds(0, 7)], r2b.at[k - 1, :, pl.ds(0, 7)], other_x[k]) for k in XORDER]
    arrived(t4)
    g2[x] = g1[...]
    t5 = [put(g2.at[x], g2.at[x], other_x[k]) for k in XORDER]
    arrived(p2b)
    total = s2b[pl.ds(x * 8, 8), 0:7]
    for part in range(3):
        total = total + r2b[part, :, 0:7]
    s3b[:, 0:7] = total
    p3b = [put(s3b.at[(v + k) % 8, pl.ds(0, 7)], r3b.at[k - 1, pl.ds(0, 7)], other_v[k]) for k in ORDER]
    arrived(p2a)
    total = s2a[pl.ds(u * 64, 64), :]
    for part in range(7):
        total = total + r2a[part]
    s3a[...] = total
    p3a = [put(s3a.at[pl.ds(((v + k) % 8) * 8, 8)], r3a.at[k - 1], other_v[k]) for k in ORDER]

    arrived(t5)
    t6 = put(g2, g3, mate)
    arrived(p3b)
    lower = s3b[v, 0:7]
    for part in range(7):
        lower = lower + r3b[part, 0:7]
    lower = jnp.concatenate([lower, jnp.zeros((1, 128), f32)], axis=0)
    arrived(p3a)
    upper = s3a[pl.ds(v * 8, 8), :]
    for part in range(7):
        upper = upper + r3a[part]
    gx, gy = lax.axis_index("gx"), lax.axis_index("gy")
    offset = ((gx * 16 + gy) * 1775) % 128
    turned = pltpu.roll(jnp.concatenate([upper, lower], axis=0), (128 - offset) % 128, 1)
    below = pltpu.roll(turned, 15, 0)
    lane = lax.broadcasted_iota(jnp.int32, (16, 128), 1)
    out[...] = jnp.where(lane < 128 - offset, turned, below)

    top[256:257, 0:128] = extra[0:1]
    top[256:257, 128:256] = extra[1:2]
    top[257:258, 0:128] = extra[2:3]
    top[257:258, 128:256] = extra[3:4]
    arrived([t6])

    @pl.when(core == 0)
    def _():
        top[0:256, 0:128] = g2[...].reshape(256, 128)
        top[0:256, 128:256] = g3[...].reshape(256, 128)

    @pl.when(core == 1)
    def _():
        top[0:256, 128:256] = g2[...].reshape(256, 128)
        top[0:256, 0:128] = g3[...].reshape(256, 128)

    for copy in copies:
        copy.wait_send()


def step(*args):
    bf16, f32, i32 = jnp.bfloat16, jnp.float32, jnp.int32
    kinds = [jax.typeof(arg) for arg in args]
    vmem = pl.BlockSpec(memory_space=pltpu.VMEM)
    wide = [128, 4096, 256, 256, 512, 128, 512, None, 256]
    shapes = [(2048,), (256, 8), (2048,), (256, 8), (2, 512), (7, 32, 8), (512,), (32, 8), (7, 64), (3, 8, 8), (64,), (8, 8),
              (7, 8), (7, 8),
              (256,), (8,), (4, 72), (4, 72), (8, 16), (8, 16), (8, 16), (8, 8), (4, 8, 8), (4, 8, 8), (2, 256), (2, 16, 8)]
    scratch = [pltpu.VMEM(kind.shape, kind.dtype) for kind in kinds] + [pltpu.SemaphoreType.DMA((12,))]
    scratch += [pltpu.VMEM(shape + (128,), f32) for shape in ((2, 2048), (2, 256, 8), (2, 256), (8,))]
    scratch += [pltpu.VMEM((count, 256), f32) if count else pltpu.VMEM((2, 4096, 256), bf16) for count in wide]
    scratch += [pltpu.VMEM(shape + (128,), f32) for shape in [(7312,), (2, 256), (2, 1032)] + shapes]
    scratch += [pltpu.SemaphoreType.DMA((90,)), pltpu.SemaphoreType.DMA((90,))]
    return pl.pallas_call(
        step_kernel,
        out_shape=(jax.ShapeDtypeStruct((16, 128), f32), jax.ShapeDtypeStruct((258, 256), f32)),
        in_specs=[pl.BlockSpec(memory_space=pltpu.HBM)] * 12,
        out_specs=(vmem, vmem),
        scratch_shapes=scratch,
        compiler_params=pltpu.CompilerParams(collective_id=0, has_side_effects=True, vmem_limit_bytes=40 * 1024 * 1024),
        name="step",
    )(*[pltpu.with_memory_space_constraint(arg, pltpu.HBM) for arg in args])


def per_device(core_one, core_two, core_three, dense_rows, w_top, bias_top, w_out, labels, bag_ids, digit_one, digit_two,
               digit_three):
    chunk, top_grad = step(core_one, core_two, core_three, dense_rows, w_top, bias_top[None], w_out[None], labels[None],
                           bag_ids, digit_one, digit_two, digit_three)
    return (chunk.reshape(-1)[:1775], top_grad)


def solution(mesh):
    return jax.shard_map(
        per_device,
        mesh=mesh,
        in_specs=(
            P(),
            P(),
            P(),
            P(("gx", "gy"), None),
            P(),
            P(),
            P(),
            P(("gx", "gy")),
            P(("gx", "gy"), None),
            P(("gx", "gy"), None),
            P(("gx", "gy"), None),
            P(("gx", "gy"), None),
        ),
        out_specs=(P(("gx", "gy")), P()),
        check_vma=False,
    )
```

```python
import functools

import jax
import jax.numpy as jnp
from jax import lax
from jax.experimental import pallas as pl
from jax.experimental.pallas import tpu as pltpu
from jax.sharding import PartitionSpec as P

MESH = pl.DeviceIdType.MESH
ORDER = (1, 7, 2, 6, 3, 5, 4)
XORDER = (1, 3, 2)


def whereabouts():
    gx, gy = lax.axis_index("gx"), lax.axis_index("gy")
    core, x = gx % 2, (gx // 2) % 4
    y, z = gy % 8, (gx // 8) * 2 + gy // 8
    u = (1 - core) * y + core * z
    v = (1 - core) * z + core * y
    return core, x, u, v


def place(core, x, u, v):
    y = (1 - core) * u + core * v
    z = core * u + (1 - core) * v
    return ((z // 2) * 8 + x * 2 + core, (z % 2) * 8 + y)


def summed(rows, step, store, *parts):
    def body(i, carry):
        at = pl.ds(pl.multiple_of(i * step, step), step)
        total = parts[0](at)
        for part in parts[1:]:
            total = total + part(at)
        store(at, total)
        return carry

    lax.fori_loop(0, rows // step, body, 0)


def contract(a, b, left, right, **kw):
    return lax.dot_general(a, b, (((left,), (right,)), ((), ())), preferred_element_type=jnp.float32, **kw)


def halves(value):
    high = value.astype(jnp.bfloat16)
    return high, (value - high.astype(jnp.float32)).astype(jnp.bfloat16)


def step_kernel(*refs):
    sources, (out, top), rest = refs[:12], refs[12:14], refs[14:]
    inputs, sems, rest = rest[:12], rest[12], rest[13:]
    one, two, three, dense, w_top, bias, w_out, labels, bags, digit_one, digit_two, digit_three = inputs
    (wa, wb, t, e, first, mid, last, turned, left, g, gl, gm, glast, flat, sided, gf) = rest[:16]
    (r0a, r0b, s1a, s1b, r1a, r1b, s2a, s2b, r2a, r2b, s3a, s3b, r3a, r3b, rt0, re0, st1, rt1, st2, rt2, rt3, g1, g2, g3, rel_a, rel_b,
     send, recv) = rest[16:]
    loads = [pltpu.make_async_copy(sources[i], inputs[i], sems.at[i]) for i in range(12)]
    for i in (9, 11, 10, 0, 2, 1, 8, 3, 4, 5, 6, 7):
        loads[i].start()
    core, x, u, v = whereabouts()
    y = (1 - core) * u + core * v
    z = core * u + (1 - core) * v
    mate = ((z // 2) * 8 + x * 2 + (1 - core), (z % 2) * 8 + y)
    other_x = {k: place(core, (x + k) % 4, u, v) for k in XORDER}
    other_u = {k: place(core, x, (u + k) % 8, v) for k in ORDER}
    other_v = {k: place(core, x, u, (v + k) % 8) for k in ORDER}
    barrier = pltpu.get_barrier_semaphore()
    peers = [mate] + list(other_x.values()) + list(other_u.values()) + list(other_v.values())
    for peer in peers:
        pl.semaphore_signal(barrier, inc=1, device_id=peer, device_id_type=MESH)
    copies = []

    def put(src, dst, peer):
        spot = len(copies)
        copy = pltpu.make_async_remote_copy(
            src_ref=src, dst_ref=dst, send_sem=send.at[spot], recv_sem=recv.at[spot],
            device_id=peer, device_id_type=MESH)
        copy.start()
        copies.append(copy)
        return copy

    def arrived(group):
        for copy in group:
            copy.wait_recv()

    for i in (9, 0, 11, 2, 10, 8):
        loads[i].wait()
    bf16, f32 = jnp.bfloat16, jnp.float32

    def hot(row, count, kind):
        return (lax.broadcasted_iota(jnp.int32, (count, row.shape[1]), 0) == row).astype(kind)

    hot_one = hot(digit_one[...], 200, bf16)
    first[...] = contract(one[...], hot_one, 0, 0)
    hot_three = hot(digit_three[...], 250, bf16)
    ends = contract(three[...], hot_three, 0, 0)
    last[...] = ends
    for side in range(2):
        sided[side] = ends[:, side * 128:side * 128 + 128]
        for d in range(8):
            turned[d * 32:d * 32 + 32, side * 128:side * 128 + 128] = sided.at[side][pl.ds(d, 32, stride=8), :]
    hot_two = hot(digit_two[...], 200, bf16)
    bag = hot(bags[...], 64, bf16)
    loads[1].wait()
    for part in range(8):
        mid[part * 512:part * 512 + 512, :] = contract(two[:, part * 512:part * 512 + 512], hot_two, 0, 0)

    for b in range(4):
        sums = [jnp.zeros((32, 256), f32) for _ in range(4)]
        for a in range(32):
            piece = mid[a * 128 + b * 32:a * 128 + b * 32 + 32, :]
            sums = [total + first[i * 32 + a:i * 32 + a + 1, :] * piece for i, total in enumerate(sums)]
        for i in range(4):
            left[(i * 4 + b) * 32:(i * 4 + b) * 32 + 32, :] = sums[i]
    rows = []
    for p in range(16):
        total = jnp.zeros((8, 256), f32)
        for a in range(32):
            total = total + left[p * 32 + a:p * 32 + a + 1, :] * last[a * 8:a * 8 + 8, :]
        rows.append(total)
    embedded = jnp.concatenate(rows, axis=0)

    for i in (3, 4, 5, 6, 7):
        loads[i].wait()
    upper, lower = halves(embedded)
    pooled = contract(bag, upper, 1, 1) + contract(bag, lower, 1, 1)
    joined = jnp.concatenate([dense[...], pooled.astype(bf16)], axis=1)
    pre = jnp.dot(joined, w_top[...], preferred_element_type=f32) + bias[...]
    sig = jax.nn.sigmoid(pre)
    hidden = pre * sig
    logit = jnp.sum(hidden * w_out[...], axis=1, keepdims=True)
    square = lax.broadcasted_iota(jnp.int32, (64, 64), 0) == lax.broadcasted_iota(jnp.int32, (64, 64), 1)
    label = jnp.sum(jnp.where(square, labels[...].astype(f32), 0.0), axis=1, keepdims=True)
    dlogit = (jax.nn.sigmoid(logit) - label) / 64
    dpre = dlogit * w_out[...] * (sig * (1.0 + pre * (1.0 - sig)))
    low = dpre.astype(bf16)
    weight = contract(joined, low, 0, 0)
    t[0] = weight[:, 0:128]
    t[1] = weight[:, 128:256]
    grad_bias = jnp.sum(dpre, axis=0, keepdims=True)
    grad_out = jnp.sum(hidden * dlogit, axis=0, keepdims=True)
    e[...] = jnp.concatenate([grad_bias[:, :128], grad_bias[:, 128:], grad_out[:, :128], grad_out[:, 128:],
                              jnp.zeros((4, 128), f32)], axis=0)
    pooled_grad = contract(w_top[128:256, :], low, 1, 1)
    upper, lower = halves(pooled_grad)
    g[...] = contract(upper, bag, 1, 0) + contract(lower, bag, 1, 0)

    pl.semaphore_wait(barrier, len(peers))
    t0 = [put(t.at[1 - core], rt0, mate), put(e, re0, mate)]

    for a in range(32):
        total = jnp.zeros((8, 256), f32)
        for p in range(16):
            total = total + left[p * 32 + a:p * 32 + a + 1, :] * g[p * 8:p * 8 + 8, :]
        glast[a * 8:a * 8 + 8, :] = total
    for p in range(16):
        total = jnp.zeros((32, 256), f32)
        for d in range(8):
            total = total + g[p * 8 + d:p * 8 + d + 1, :] * turned[d * 32:d * 32 + 32, :]
        gl[p * 32:p * 32 + 32, :] = total

    def scatter(table, value):
        upper, lower = halves(value)
        return contract(table, upper, 1, 1) + contract(table, lower, 1, 1)

    def middles(low_a, high_a):
        for a in range(low_a, high_a, 2):
            for c in (a, a + 1):
                partial = [jnp.zeros((8, 256), f32) for _ in range(4)]
                scale = [jnp.broadcast_to(first[i * 32 + c:i * 32 + c + 1, :], (8, 256)) for i in range(4)]
                for b in range(8):
                    totals = []
                    for at in (c * 128 + b * 16, c * 128 + b * 16 + 8):
                        piece = mid[at:at + 8, :]
                        total = None
                        for i in range(4):
                            low_at = i * 128 + at - c * 128
                            slope = gl[low_at:low_at + 8, :]
                            total = scale[i] * slope if total is None else total + scale[i] * slope
                            partial[i] = partial[i] + slope * piece
                        totals.append(total)
                    upper, lower = halves(jnp.concatenate(totals, axis=0))
                    gm[0, c * 128 + b * 16:c * 128 + b * 16 + 16, :] = upper
                    gm[1, c * 128 + b * 16:c * 128 + b * 16 + 16, :] = lower
                for i in range(4):
                    for side in range(2):
                        gf.at[side][pl.ds(i * 32 + c, 8, stride=129), :] = partial[i][:, side * 128:side * 128 + 128]
            middle = contract(hot_two, gm[0, a * 128:a * 128 + 256, :], 1, 1)
            middle = middle + contract(hot_two, gm[1, a * 128:a * 128 + 256, :], 1, 1)
            flat[pl.ds(200 + a, 200, stride=33), :] = middle[:, 0:128]
            flat[pl.ds(201 + a, 200, stride=33), :] = middle[:, 128:256]

    middles(0, 16)
    arrived(t0)
    extra = e[...] + re0[...]
    for part in range(4):
        rows = pl.ds(part * 64, 64)
        st1[part, 0:64, :] = t[core, rows, :] + rt0[rows, :]
        st1[part, 64:72, :] = extra
    t1 = [put(st1.at[(x + k) % 4], rt1.at[x], other_x[k]) for k in XORDER]
    rt1[x] = st1[x]

    ending = scatter(hot_three, glast[...])
    flat[pl.ds(6800, 250, stride=2), :] = ending[:, 0:128]
    flat[pl.ds(6801, 250, stride=2), :] = ending[:, 128:256]
    middles(16, 32)
    total = jnp.zeros((200, 128), f32)
    for part in range(0, 8, 2):
        pieces = [gf[side, at * 129:at * 129 + 128, :] for at in (part, part + 1) for side in (0, 1)]
        spread = scatter(hot_one, jnp.concatenate([jnp.concatenate(pieces[:2], axis=1), jnp.concatenate(pieces[2:], axis=1)], axis=0))
        total = total + spread[:, 0:128] + spread[:, 128:256]
    flat[0:200, :] = total
    flat[7300:7312, :] = jnp.zeros((12, 128), f32)

    def rows_from(start):
        spans, at = [], start
        while at < start + 8:
            if at < 200:
                size, place_at = min(200 - at, start + 8 - at), at
            elif at < 6600:
                size, place_at = min(32 - (at - 200) % 32, start + 8 - at), 200 + (at - 200) // 32 * 33 + (at - 200) % 32
            else:
                size, place_at = start + 8 - at, at + 200
            spans.append((at - start, size, place_at))
            at += size
        return spans

    def packed(color):
        for q in range(512):
            side, qx, qy = (q // 16) % 2, (q // 32) % 4, q % 8
            qz = (q // 128) * 2 + (q // 8) % 2
            qu, qv = (qy, qz) if side == 0 else (qz, qy)
            slot = qx * 64 + qu * 8 + qv if color == 0 else qu * 32 + qx * 8 + qv
            for shift, size, place_at in rows_from((1775 * q) // 128 + 8 * color):
                if color == 0:
                    wa[side, slot * 8 + shift:slot * 8 + shift + size, :] = flat[place_at:place_at + size, :]
                else:
                    wb[side, slot, shift:shift + size, :] = flat[place_at:place_at + size, :]

    plan = ((0, 2), (1, 4), (1, 3), (1, 5), (0, 1), (0, 3), (1, 2), (1, 6), (1, 1), (1, 7), (0, 0), (1, 0))

    def piece_of(color, distance, x_at, u_at):
        return pl.ds(((x_at + distance) % 4) * 512, 512) if color == 0 else pl.ds(((u_at + distance) % 8) * 32, 32)

    p0 = {}
    def pair_copies(wanted):
        for color, distance in wanted:
            rows = piece_of(color, distance, x, v)
            if color == 0:
                p0[color, distance] = put(wa.at[1 - core, rows], r0a.at[rows], mate)
            else:
                p0[color, distance] = put(wb.at[1 - core, rows, pl.ds(0, 7)], r0b.at[rows, pl.ds(0, 7)], mate)

    packed(0)
    pair_copies(plan[:1])
    packed(1)
    pair_copies(plan[1:])
    arrived(t1)
    total = rt1[0]
    for part in range(1, 4):
        total = total + rt1[part]
    for part in range(8):
        st2[part, 0:8, :] = total[part * 8:part * 8 + 8]
        st2[part, 8:16, :] = total[64:72]
    t2 = [put(st2.at[(v + k) % 8], rt2.at[v], other_v[k]) for k in ORDER]
    rt2[v] = st2[v]

    def fold(color, distance):
        p0[color, distance].wait_recv()
        rows = piece_of(color, distance, x, u)
        if color == 0:
            s1a[rows, :] = wa[core, rows, :] + r0a[rows, :]
        else:
            s1b[rows, 0:7] = wb[core, rows, 0:7] + r0b[rows, 0:7]

    def part_a(slot, half):
        return s1a.at[pl.ds(slot * 512 + half * 256, 256)]

    def part_b(slot, start=0, size=32):
        return s1b.at[pl.ds(slot * 32 + start, size), pl.ds(0, 7)]

    def land_b(k, start=0, size=32):
        return r1b.at[k - 1, pl.ds(start, size), pl.ds(0, 7)]

    def relayed_a(slot, half, came):
        at = pl.ds(slot * 512 + half * 256, 256)
        s1a[at, :] = s1a[at, :] + came[...]

    def relayed_b(slot, half, way):
        at = pl.ds(slot * 32 + half * 16, 16)
        s1b[at, 0:7] = s1b[at, 0:7] + rel_b[way, :, 0:7]

    far, across = (u + 4) % 8, (x + 2) % 4
    fold(0, 2)
    relay_a = [put(part_a(across, 0), rel_a.at[0], other_x[1]), put(part_a(across, 1), rel_a.at[1], other_x[3])]
    fold(1, 4)
    relay_b = [put(part_b(far, 0, 16), rel_b.at[0, :, pl.ds(0, 7)], other_u[2]), put(part_b(far, 16, 16), rel_b.at[1, :, pl.ds(0, 7)], other_u[6])]
    p1a, p1b = [], []
    for k in (3, 5):
        fold(1, k)
        p1b.append(put(part_b((u + k) % 8), land_b(k), other_u[k]))
    fold(0, 1)
    p1a.append(put(part_a((x + 1) % 4, 1), r1a.at[0, pl.ds(256, 256)], other_x[1]))
    fold(0, 3)
    p1a.append(put(part_a((x + 3) % 4, 0), r1a.at[1, pl.ds(0, 256)], other_x[3]))
    fold(1, 2)
    p1b.append(put(part_b((u + 2) % 8, 16, 16), land_b(2, 16, 16), other_u[2]))
    fold(1, 6)
    p1b.append(put(part_b((u + 6) % 8, 0, 16), land_b(6, 0, 16), other_u[6]))
    arrived(t2)
    total = rt2[0]
    for part in range(1, 8):
        total = total + rt2[part]
    rt3[u] = total
    t3 = [put(rt3.at[u], rt3.at[u], other_u[k]) for k in ORDER]
    for k in (1, 7):
        fold(1, k)
        p1b.append(put(part_b((u + k) % 8), land_b(k), other_u[k]))
    fold(0, 0)
    fold(1, 0)
    arrived(relay_b)
    relayed_b((u + 2) % 8, 0, 0)
    relayed_b((u + 6) % 8, 1, 1)
    p1b += [put(part_b((u + 2) % 8, 0, 16), land_b(2, 0, 16), other_u[2]),
            put(part_b((u + 6) % 8, 16, 16), land_b(6, 16, 16), other_u[6])]
    arrived(relay_a)
    relayed_a((x + 1) % 4, 0, rel_a.at[0])
    relayed_a((x + 3) % 4, 1, rel_a.at[1])
    p1a += [put(part_a((x + 1) % 4, 0), r1a.at[0, pl.ds(0, 256)], other_x[1]),
            put(part_a((x + 3) % 4, 1), r1a.at[1, pl.ds(256, 256)], other_x[3])]

    arrived(p1a)

    def store2a(at, value):
        s2a[at, :] = value

    summed(512, 128, store2a, lambda at: s1a[pl.ds(x * 512 + at.start, at.size), :],
           *[functools.partial(lambda k, at: r1a[k, at, :], k) for k in range(2)])
    p2a = [put(s2a.at[pl.ds(((u + k) % 8) * 64, 64)], r2a.at[k - 1], other_u[k]) for k in ORDER]
    arrived(t3)
    total = rt3[0]
    for part in range(1, 8):
        total = total + rt3[part]
    g1[v] = total[0:8]
    extra = total[8:16]
    t4 = [put(g1.at[v], g1.at[v], other_v[k]) for k in ORDER]
    arrived(p1b)

    def fold2(part, carry):
        at = pl.ds(pl.multiple_of(part * 8, 8), 8)
        total = s1b[pl.ds(u * 32 + part * 8, 8), 0:7]
        for k in (1, 2, 3, 5, 6, 7):
            total = total + r1b[k - 1, at, 0:7]
        s2b[at, 0:7] = total
        return carry

    lax.fori_loop(0, 4, fold2, 0)
    p2b = [put(s2b.at[pl.ds(((x + k) % 4) * 8, 8), pl.ds(0, 7)], r2b.at[k - 1, :, pl.ds(0, 7)], other_x[k]) for k in XORDER]
    arrived(t4)
    g2[x] = g1[...]
    t5 = [put(g2.at[x], g2.at[x], other_x[k]) for k in XORDER]
    arrived(p2b)
    total = s2b[pl.ds(x * 8, 8), 0:7]
    for part in range(3):
        total = total + r2b[part, :, 0:7]
    s3b[:, 0:7] = total
    p3b = [put(s3b.at[(v + k) % 8, pl.ds(0, 7)], r3b.at[k - 1, pl.ds(0, 7)], other_v[k]) for k in ORDER]
    arrived(p2a)
    total = s2a[pl.ds(u * 64, 64), :]
    for part in range(7):
        total = total + r2a[part]
    s3a[...] = total
    p3a = [put(s3a.at[pl.ds(((v + k) % 8) * 8, 8)], r3a.at[k - 1], other_v[k]) for k in ORDER]

    arrived(t5)
    t6 = put(g2, g3, mate)
    arrived(p3b)
    lower = s3b[v, 0:7]
    for part in range(7):
        lower = lower + r3b[part, 0:7]
    lower = jnp.concatenate([lower, jnp.zeros((1, 128), f32)], axis=0)
    arrived(p3a)
    upper = s3a[pl.ds(v * 8, 8), :]
    for part in range(7):
        upper = upper + r3a[part]
    gx, gy = lax.axis_index("gx"), lax.axis_index("gy")
    offset = ((gx * 16 + gy) * 1775) % 128
    turned = pltpu.roll(jnp.concatenate([upper, lower], axis=0), (128 - offset) % 128, 1)
    below = pltpu.roll(turned, 15, 0)
    lane = lax.broadcasted_iota(jnp.int32, (16, 128), 1)
    out[...] = jnp.where(lane < 128 - offset, turned, below)

    top[256:257, 0:128] = extra[0:1]
    top[256:257, 128:256] = extra[1:2]
    top[257:258, 0:128] = extra[2:3]
    top[257:258, 128:256] = extra[3:4]
    arrived([t6])

    @pl.when(core == 0)
    def _():
        top[0:256, 0:128] = g2[...].reshape(256, 128)
        top[0:256, 128:256] = g3[...].reshape(256, 128)

    @pl.when(core == 1)
    def _():
        top[0:256, 128:256] = g2[...].reshape(256, 128)
        top[0:256, 0:128] = g3[...].reshape(256, 128)

    for copy in copies:
        copy.wait_send()


def step(*args):
    bf16, f32, i32 = jnp.bfloat16, jnp.float32, jnp.int32
    kinds = [jax.typeof(arg) for arg in args]
    vmem = pl.BlockSpec(memory_space=pltpu.VMEM)
    wide = [128, 4096, 256, 256, 512, 128, 512, None, 256]
    shapes = [(2048,), (256, 8), (2048,), (256, 8), (2, 512), (7, 32, 8), (512,), (32, 8), (7, 64), (3, 8, 8), (64,), (8, 8),
              (7, 8), (7, 8),
              (256,), (8,), (4, 72), (4, 72), (8, 16), (8, 16), (8, 16), (8, 8), (4, 8, 8), (4, 8, 8), (2, 256), (2, 16, 8)]
    scratch = [pltpu.VMEM(kind.shape, kind.dtype) for kind in kinds] + [pltpu.SemaphoreType.DMA((12,))]
    scratch += [pltpu.VMEM(shape + (128,), f32) for shape in ((2, 2048), (2, 256, 8), (2, 256), (8,))]
    scratch += [pltpu.VMEM((count, 256), f32) if count else pltpu.VMEM((2, 4096, 256), bf16) for count in wide]
    scratch += [pltpu.VMEM(shape + (128,), f32) for shape in [(7312,), (2, 256), (2, 1032)] + shapes]
    scratch += [pltpu.SemaphoreType.DMA((90,)), pltpu.SemaphoreType.DMA((90,))]
    return pl.pallas_call(
        step_kernel,
        out_shape=(jax.ShapeDtypeStruct((16, 128), f32), jax.ShapeDtypeStruct((258, 256), f32)),
        in_specs=[pl.BlockSpec(memory_space=pltpu.HBM)] * 12,
        out_specs=(vmem, vmem),
        scratch_shapes=scratch,
        compiler_params=pltpu.CompilerParams(collective_id=0, has_side_effects=True, vmem_limit_bytes=40 * 1024 * 1024),
        name="step",
    )(*[pltpu.with_memory_space_constraint(arg, pltpu.HBM) for arg in args])


def per_device(core_one, core_two, core_three, dense_rows, w_top, bias_top, w_out, labels, bag_ids, digit_one, digit_two,
               digit_three):
    chunk, top_grad = step(core_one, core_two, core_three, dense_rows, w_top, bias_top[None], w_out[None], labels[None],
                           bag_ids, digit_one, digit_two, digit_three)
    return (chunk.reshape(-1)[:1775], top_grad)


def solution(mesh):
    return jax.shard_map(
        per_device,
        mesh=mesh,
        in_specs=(
            P(),
            P(),
            P(),
            P(("gx", "gy"), None),
            P(),
            P(),
            P(),
            P(("gx", "gy")),
            P(("gx", "gy"), None),
            P(("gx", "gy"), None),
            P(("gx", "gy"), None),
            P(("gx", "gy"), None),
        ),
        out_specs=(P(("gx", "gy")), P()),
        check_vma=False,
    )
```
